128 devices in a mesh: bx: 16 (over z, x), by: 8 (over y, core).
Axes of the slice: x: 4, y: 4, z: 4, core: 2. Of those that a mesh axis runs over, the one named last changes fastest.
Arguments:
- layer_temps: float32 [40, 1024, 4096], P(None, 'by', 'bx'), may hold values from -12 to -2
- ice_thick: float32 [5, 1024, 4096], P(None, 'by', 'bx'), may hold values from 0.5 to 3
- snow_thick: float32 [5, 1024, 4096], P(None, 'by', 'bx'), may hold values from 0.05 to 0.5
- ice_area: float32 [5, 1024, 4096], P(None, 'by', 'bx'), may hold values from 0.12 to 0.2
- air_temp: float32 [1024, 4096], P('by', 'bx'), may hold values from -30 to -5
- ocean_heat: float32 [1024, 4096], P('by', 'bx'), may hold values from 0 to 300
- velocity: float32 [2, 1024, 4096], P(None, 'by', 'bx'), may hold values from -3 to 3
- stress: float32 [3, 1024, 4096], P(None, 'by', 'bx'), may hold values from -2 to 2
- wind_stress: float32 [2, 1024, 4096], P(None, 'by', 'bx'), may hold values from -5 to 5
- ocean_current: float32 [2, 1024, 4096], P(None, 'by', 'bx'), may hold values from -2 to 2
- ocean_mask: int32 [1024, 4096], P('by', 'bx'), may hold values 0 or 1
- ice_cols: int32 [8, 16, 6144], P('by', 'bx'), may hold values from -1 to 32767, as said below
Outputs:
- layer_temps_new: float32 [40, 1024, 4096], P(None, 'by', 'bx')
- ice_thick_new: float32 [5, 1024, 4096], P(None, 'by', 'bx')
- velocity_new: float32 [2, 1024, 4096], P(None, 'by', 'bx')
- stress_new: float32 [3, 1024, 4096], P(None, 'by', 'bx')
The draws below stay inside these ranges and needn't reach their ends.
Inputs may be any that keep to these rules, and one draw needn't show every extreme that they name: `ice_cols`: each block's 6144 slots list its ice-covered cells first, each cell once, as e = row * 256 + column inside the block, and hold -1 in every later slot. All blocks together list exactly 2048 times the number of blocks cells, and some block lists 6144 cells.
All inputs are finite; a program needn't handle non-finite values. No bound on the sum of `ocean_mask` on one device may be relied on, other than what follows from the above.
Results may differ from the reference program's by a relative error of at most 0.0001.
Values sent between devices are 32-bit elements; how exact they have to be, the bound alone decides.
No kernel may reach another device: no remote copies, remote signals or barrier semaphores. Data moves between devices by JAX's collectives and lax.ppermute only.
A program may use at most 192 MiB of HBM per device.

```python
import jax
import jax.numpy as jnp
from jax import lax

CATS = 5
LAYERS = 8
ITERS = 4
SUB = 4
CY = 128
CX = 256
LIVE_DEV = 2048
CMAX = 6144
NY = 1024
NX = 4096
N_BX = 16
N_BY = 8


def draw_ice_cols(key, part):
    blocks = N_BY * N_BX
    cells = CY * CX
    level_key, full_key, order_key, cell_key = jax.random.split(jax.random.fold_in(key, 17), 4)
    levels = jax.random.randint(level_key, (blocks,), 0, 4)
    full_block = jax.random.randint(full_key, (), 0, blocks)
    block_ids = jnp.arange(blocks)
    limits = jnp.where(block_ids == full_block, 0, (levels + 2) * CMAX // 5)
    slot_ids = jnp.arange(CMAX)
    eligible = (slot_ids[None, :] < limits[:, None]).reshape(-1)
    shuffled = jax.random.permutation(order_key, blocks * CMAX)
    inverse = jnp.argsort(shuffled)
    scores = jnp.where(eligible, inverse, blocks * CMAX + jnp.arange(blocks * CMAX))
    placed = jnp.argsort(jnp.argsort(scores))
    chosen = (placed < blocks * LIVE_DEV - CMAX).reshape(blocks, CMAX)
    counts = jnp.sum(chosen.astype(jnp.int32), axis=1) + jnp.where(block_ids == full_block, CMAX, 0)
    orders = jax.vmap(lambda sub_key: jax.random.permutation(sub_key, cells))(jax.random.split(cell_key, blocks))[:, :CMAX]
    listed = jnp.where(slot_ids[None, :] < counts[:, None], orders, -1)
    return listed.astype(jnp.int32).reshape(N_BY, N_BX, CMAX)


def with_ends(values, stream_key, least, high):
    longest = values.shape.index(max(values.shape))
    spots = []
    for shift in (0, 1):
        where = [jax.random.randint(jax.random.fold_in(stream_key, axis), (), 0, length) for axis, length in enumerate(values.shape)]
        where[longest] = (where[longest] + shift) % values.shape[longest]
        spots.append(tuple(where))
    return values.at[spots[0]].set(least).at[spots[1]].set(high)


def level_of(own_key, extent, cuts, low, top_value):
    loudness, own = 1.0, jax.random.fold_in(own_key, 6)
    for position, shards_of in cuts:
        steps = jnp.exp(jax.random.uniform(jax.random.fold_in(own, position), (shards_of,), jnp.float32, low / len(cuts), top_value / len(cuts)))
        loudness = loudness * jnp.repeat(steps, extent[position] // shards_of).reshape([-1 if axis == position else 1 for axis in range(len(extent))])
    return loudness


def gaussian(key, shape, deviation, bound, cuts=(), held_as=jnp.bfloat16):
    gain = level_of(key, shape, cuts, -0.22, 0.18) if cuts else 1.0
    values = jax.random.normal(key, shape, jnp.float32) * deviation * gain
    return jnp.minimum(jnp.maximum(values, -bound), bound).astype(held_as)


def setup_inputs(seed: int = 0) -> dict:
    key_of = jax.random.split(jax.random.key(seed), 13)
    layer_temps = jnp.clip(-12.0 + 10.0 * jax.random.uniform(key_of[0], (CATS * LAYERS, NY, NX), jnp.float32) ** level_of(key_of[0], (CATS * LAYERS, NY, NX), ((1, 8), (2, 16)), -0.2, 0.2), -12.0, -2.0)
    ice_thick = jnp.clip(0.5 + 2.5 * jax.random.uniform(key_of[1], (CATS, NY, NX), jnp.float32) ** level_of(key_of[1], (CATS, NY, NX), ((1, 8), (2, 16)), -0.2, 0.2), 0.5, 3.0)
    snow_thick = jnp.clip(0.05 + 0.45 * jax.random.uniform(key_of[2], (CATS, NY, NX), jnp.float32) ** level_of(key_of[2], (CATS, NY, NX), ((1, 8), (2, 16)), -0.2, 0.2), 0.05, 0.5)
    ice_area = jnp.clip(0.12 + 0.080000006 * jax.random.uniform(key_of[3], (CATS, NY, NX), jnp.float32) ** level_of(key_of[3], (CATS, NY, NX), ((1, 8), (2, 16)), -0.2, 0.2), 0.12, 0.2)
    air_temp = jnp.clip(-30.0 + 25.0 * jax.random.uniform(key_of[4], (NY, NX), jnp.float32) ** level_of(key_of[4], (NY, NX), ((0, 8), (1, 16)), -0.2, 0.2), -30.0, -5.0)
    ocean_heat = jnp.clip(300.0 * jax.random.uniform(key_of[5], (NY, NX), jnp.float32) ** level_of(key_of[5], (NY, NX), ((0, 8), (1, 16)), -0.2, 0.2), 0.0, 300.0)
    velocity = gaussian(key_of[6], (2, NY, NX), 0.5, 3.0, ((1, 8), (2, 16)), jnp.float32)
    stress = gaussian(key_of[7], (3, NY, NX), 0.3, 2.0, ((1, 8), (2, 16)), jnp.float32)
    wind_stress = gaussian(key_of[8], (2, NY, NX), 1.0, 5.0, ((1, 8), (2, 16)), jnp.float32)
    ocean_current = gaussian(key_of[9], (2, NY, NX), 0.3, 2.0, ((1, 8), (2, 16)), jnp.float32)
    ocean_mask = with_ends((jax.random.randint(key_of[10], (NY, NX), 0, 10) < 9).astype(jnp.int32), jax.random.fold_in(key_of[10], 1), 0, 1)
    ice_cols = draw_ice_cols(jax.random.fold_in(key_of[12], 71), 0)
    return dict(layer_temps=layer_temps, ice_thick=ice_thick, snow_thick=snow_thick, ice_area=ice_area, air_temp=air_temp, ocean_heat=ocean_heat, velocity=velocity, stress=stress, wind_stress=wind_stress, ocean_current=ocean_current, ocean_mask=ocean_mask, ice_cols=ice_cols)


FREEZING = -1.8
THERMO_STEP = 0.1
AIR_EXCHANGE = 20.0
GROWTH_RATE = 0.0005
RELAX = 0.5
DRAG = 1.0
DENSITY = 0.9
HARDENING = 20.0

def solve_layers(diagonal, coupling, right_side):
    ratios = [coupling[0] / diagonal[0]]
    values = [right_side[0] / diagonal[0]]
    for layer_pos in range(1, len(diagonal)):
        denom = diagonal[layer_pos] - coupling[layer_pos - 1] * ratios[layer_pos - 1]
        if layer_pos < len(diagonal) - 1:
            ratios.append(coupling[layer_pos] / denom)
        values.append((right_side[layer_pos] + coupling[layer_pos - 1] * values[layer_pos - 1]) / denom)
    result = [values[-1]]
    for layer_pos in range(len(diagonal) - 2, -1, -1):
        result.insert(0, values[layer_pos] + ratios[layer_pos] * result[0])
    return result

def conductivity(current, layers, snow):
    return [jnp.full_like(snow, 0.31)] + [2.03 + 0.47 / (1.0 + current[layer_pos] * current[layer_pos]) for layer_pos in range(1, layers)]

def column_physics(packed, categories, layers):
    width = packed.shape[1]
    stacked = categories * layers
    temps = packed[:stacked].reshape(categories, layers, width)
    thick = packed[stacked:stacked + categories]
    snow = packed[stacked + categories:stacked + 2 * categories]
    air = packed[stacked + 2 * categories]
    heat = packed[stacked + 2 * categories + 1]
    depth = [snow] + [thick / (layers - 1)] * (layers - 1)
    start = [temps[:, layer_pos] for layer_pos in range(layers)]
    current = start
    for repeat in range(ITERS):
        conduct = conductivity(current, layers, snow)
        capacity = [2.1 * depth[0] / THERMO_STEP] + [(2.1 + 72.0 / (1.0 + current[layer_pos] * current[layer_pos])) * depth[layer_pos] / THERMO_STEP for layer_pos in range(1, layers)]
        inner = [2.0 / (depth[layer_pos] / conduct[layer_pos] + depth[layer_pos + 1] / conduct[layer_pos + 1]) for layer_pos in range(layers - 1)]
        top_link = 1.0 / (1.0 / AIR_EXCHANGE + 0.5 * depth[0] / conduct[0])
        base_link = 2.0 * conduct[-1] / depth[-1]
        links = [top_link] + inner + [base_link]
        diagonal = [capacity[layer_pos] + links[layer_pos] + links[layer_pos + 1] for layer_pos in range(layers)]
        right_side = [capacity[layer_pos] * start[layer_pos] for layer_pos in range(layers)]
        right_side[0] = right_side[0] + top_link * air
        right_side[-1] = right_side[-1] + base_link * FREEZING
        current = solve_layers(diagonal, inner, right_side)
    final_link = 2.0 * conductivity(current, layers, snow)[-1] / depth[-1]
    new_thick = thick + GROWTH_RATE * (final_link * (FREEZING - current[-1]) - heat)
    new_temps = jnp.stack(current, axis=1).reshape(stacked, width)
    return jnp.concatenate([new_temps, new_thick], axis=0)

def strain_terms(east_ext, north_ext):
    east_dx = 0.5 * (east_ext[1:-1, 2:] - east_ext[1:-1, :-2])
    north_dy = 0.5 * (north_ext[2:, 1:-1] - north_ext[:-2, 1:-1])
    east_dy = 0.5 * (east_ext[2:, 1:-1] - east_ext[:-2, 1:-1])
    north_dx = 0.5 * (north_ext[1:-1, 2:] - north_ext[1:-1, :-2])
    return (east_dx + north_dy, east_dx - north_dy, east_dy + north_dx)

def relax_stress(stress_sum, stress_diff, stress_shear, strength, east_ext, north_ext):
    diverge, tension, shearing = strain_terms(east_ext, north_ext)
    deform = jnp.sqrt(diverge * diverge + 0.25 * (tension * tension + shearing * shearing) + 1.0)
    bulk = strength / deform
    shear_visc = 0.25 * bulk
    stress_sum = (stress_sum + RELAX * (bulk * diverge - strength)) / (1.0 + RELAX)
    stress_diff = (stress_diff + RELAX * shear_visc * tension) / (1.0 + RELAX)
    stress_shear = (stress_shear + RELAX * 0.5 * shear_visc * shearing) / (1.0 + RELAX)
    return (stress_sum, stress_diff, stress_shear)

def stress_force(normal_xx, normal_yy, shear_xy):
    force_east = 0.5 * (normal_xx[1:-1, 2:] - normal_xx[1:-1, :-2]) + 0.5 * (shear_xy[2:, 1:-1] - shear_xy[:-2, 1:-1])
    force_north = 0.5 * (shear_xy[1:-1, 2:] - shear_xy[1:-1, :-2]) + 0.5 * (normal_yy[2:, 1:-1] - normal_yy[:-2, 1:-1])
    return (force_east, force_north)

def momentum(east_vel, north_vel, force_east, force_north, mass, coriolis, wind_stress, ocean_current, ocean_cells):
    diagonal = mass + DRAG
    turning = coriolis * mass
    rhs_east = mass * east_vel + force_east + wind_stress[0] + DRAG * ocean_current[0]
    rhs_north = mass * north_vel + force_north + wind_stress[1] + DRAG * ocean_current[1]
    determinant = diagonal * diagonal + turning * turning
    east_new = (diagonal * rhs_east + turning * rhs_north) / determinant * ocean_cells
    north_new = (diagonal * rhs_north - turning * rhs_east) / determinant * ocean_cells
    return (east_new, north_new)

def extend_grid(fields, signs):
    wide = jnp.concatenate([fields[:, :, -1:], fields, fields[:, :, :1]], axis=2)
    north = wide[:, ::-1][:, :1][:, :, ::-1] * signs[:, None, None]
    south = jnp.zeros_like(wide[:, :1])
    return jnp.concatenate([south, wide, north], axis=1)

def reference(layer_temps, ice_thick, snow_thick, ice_area, air_temp, ocean_heat, velocity, stress, wind_stress, ocean_current, ocean_mask, ice_cols):
    cells = NY * NX
    stacked = CATS * LAYERS
    temps_flat = layer_temps.reshape(stacked, cells)
    thick_flat = ice_thick.reshape(CATS, cells)
    snow_flat = snow_thick.reshape(CATS, cells)
    air_flat = air_temp.reshape(1, cells)
    heat_flat = ocean_heat.reshape(1, cells)
    listed = ice_cols.reshape(N_BY * N_BX, CMAX).astype(jnp.int32)
    block_ids = jnp.arange(N_BY * N_BX, dtype=jnp.int32)
    block_row = (block_ids // N_BX)[:, None]
    block_col = (block_ids % N_BX)[:, None]
    safe = jnp.maximum(listed, 0)
    global_id = ((block_row * CY + safe // CX) * NX + block_col * CX + safe % CX).astype(jnp.int32)
    target = jnp.where(listed >= 0, global_id, cells).astype(jnp.int32).reshape(-1)

    def one_block(cell_ids):
        packed = jnp.concatenate([temps_flat[:, cell_ids], thick_flat[:, cell_ids], snow_flat[:, cell_ids], air_flat[:, cell_ids], heat_flat[:, cell_ids]], axis=0)
        return column_physics(packed, CATS, LAYERS)
    results = lax.map(one_block, global_id)
    results = jnp.moveaxis(results, 1, 0).reshape(stacked + CATS, -1)
    temps_new = temps_flat.at[:, target].set(results[:stacked], mode='drop').reshape(stacked, NY, NX)
    thick_new = thick_flat.at[:, target].set(results[stacked:], mode='drop').reshape(CATS, NY, NX)
    ice = jnp.zeros((cells,), jnp.float32).at[target].set(1.0, mode='drop').reshape(NY, NX)
    load = lax.optimization_barrier(jnp.sum(ice_area * thick_new, axis=0))
    area_total = lax.optimization_barrier(jnp.sum(ice_area, axis=0))
    strength = ice * load * jnp.exp(-HARDENING * (1.0 - area_total))
    mass = DENSITY * ice * load
    latitude = jnp.arange(NY).astype(jnp.float32) + 0.5
    coriolis = (1.4 * jnp.sin(0.5 * jnp.pi * (2.0 * latitude / NY - 1.0)))[:, None]
    ocean_cells = ocean_mask.astype(jnp.float32)
    flip_signs = jnp.array([-1.0, -1.0], jnp.float32)
    keep_signs = jnp.array([1.0, 1.0, 1.0], jnp.float32)
    east_vel, north_vel = (velocity[0], velocity[1])
    stress_sum, stress_diff, stress_shear = (stress[0], stress[1], stress[2])
    for subcycle in range(SUB):
        moving = extend_grid(jnp.stack([east_vel, north_vel]), flip_signs)
        stress_sum, stress_diff, stress_shear = relax_stress(stress_sum, stress_diff, stress_shear, strength, moving[0], moving[1])
        pulled = extend_grid(jnp.stack([0.5 * (stress_sum + stress_diff), 0.5 * (stress_sum - stress_diff), stress_shear]), keep_signs)
        force_east, force_north = stress_force(pulled[0], pulled[1], pulled[2])
        east_vel, north_vel = momentum(east_vel, north_vel, force_east, force_north, mass, coriolis, wind_stress, ocean_current, ocean_cells)
    return (temps_new, thick_new, jnp.stack([east_vel, north_vel]), jnp.stack([stress_sum, stress_diff, stress_shear]))
```

```python
import jax
import jax.numpy as jnp
from jax import lax
from jax.experimental import pallas as pl
from jax.experimental.pallas import tpu as pltpu
from jax.sharding import PartitionSpec as P

ITERS = 4
SUB = 4
CATS = 5
LAYERS = 8
ROWS = 128
COLS = 256
CHUNK = 8
DEEP = 8
FIELDS = 10
WIDE = COLS + 128
TALL = ROWS + 4 * DEEP
BAND = 24

FREEZING = -1.8
K_BASE = 2.03
K_GAIN = 0.47
K_SNOW = 0.31
ROOT = K_BASE / K_GAIN


def inverse(x):
    return 1.0 / x


def column(temps, thick, snow, air):
    depth = thick * (1.0 / (LAYERS - 1))
    square = depth * depth
    slope = square * (360.0 / K_GAIN)
    floor = square * (10.5 / K_GAIN)
    inv_depth = inverse(depth)
    snow_res = snow * inv_depth * (K_GAIN / K_SNOW)
    top_link = depth * (0.5 / K_GAIN) * inverse(snow * (0.5 / K_SNOW) + 0.05)
    snow_cap = snow * depth * (10.5 / K_GAIN)
    top_sum = snow_cap + top_link
    top_right = snow_cap * temps[0] + top_link * air
    current = list(temps)
    last = LAYERS - 1
    for repeat in range(ITERS):
        soft = [None] + [inverse(current[i] * current[i] + 1.0) for i in range(1, LAYERS)]
        conduct = [None] + [soft[i] + ROOT for i in range(1, LAYERS)]
        res = [snow_res] + [inverse(conduct[i]) for i in range(1, LAYERS)]
        cap = [None] + [slope * soft[i] + floor for i in range(1, LAYERS)]
        link = [res[i] + res[i + 1] for i in range(last)]
        ratio = [None] * LAYERS
        value = [None] * LAYERS
        down, down_flux = None, None
        for i in range(0, 4):
            total = top_sum if i == 0 else cap[i] + down
            right = top_right if i == 0 else cap[i] * temps[i] + down_flux
            ratio[i] = inverse(total * link[i] + 1.0)
            down = total * ratio[i]
            down_flux = right * ratio[i]
            value[i] = link[i] * down_flux
        up = conduct[last]
        up_flux = up * FREEZING
        for i in range(last, 4, -1):
            total = cap[i] + up
            right = cap[i] * temps[i] + up_flux
            ratio[i] = inverse(total * link[i - 1] + 1.0)
            up = total * ratio[i]
            up_flux = right * ratio[i]
            value[i] = link[i - 1] * up_flux
        renewed = [None] * LAYERS
        renewed[4] = (cap[4] * temps[4] + (down_flux + up_flux)) * inverse(cap[4] + (down + up))
        for i in range(3, -1, -1):
            if i > 0 or repeat == ITERS - 1:
                renewed[i] = value[i] + ratio[i] * renewed[i + 1]
        for i in range(5, LAYERS):
            renewed[i] = value[i] + ratio[i] * renewed[i - 1]
        current = renewed
    base = inverse(current[last] * current[last] + 1.0) + ROOT
    growth = (2.0 * K_GAIN * 0.0005) * (base * inv_depth) * (FREEZING - current[last])
    return current, growth


def draw_mask(list_ref, mask_ref):
    step = 512
    total = jnp.zeros((ROWS, COLS), jnp.float32)
    for start in range(0, list_ref.shape[1], step):
        cells = list_ref[:, start : start + step]
        row = lax.shift_right_arithmetic(cells, 8)
        col = jnp.where(cells >= 0, lax.bitwise_and(cells, 255), -1)
        rows = lax.broadcasted_iota(jnp.int32, (ROWS, step), 0) == row
        cols = lax.broadcasted_iota(jnp.int32, (COLS, step), 0) == col
        total = total + lax.dot_general(
            rows.astype(jnp.float32).astype(jnp.bfloat16),
            cols.astype(jnp.float32).astype(jnp.bfloat16),
            (((1,), (1,)), ((), ())),
            preferred_element_type=jnp.float32,
        )
    mask_ref[...] = total


def thermo_kernel(
    list_ref, temps_ref, thick_ref, snow_ref, area_ref, air_ref, heat_ref,
    vel_ref, stress_ref, wind_ref, ocean_ref, cells_ref,
    temps_out, thick_out, forcing_out, left_out, right_out, mask_ref,
):
    step = pl.program_id(0)

    @pl.when(step == 0)
    def _():
        draw_mask(list_ref, mask_ref)

    ice = mask_ref[pl.ds(pl.multiple_of(step * CHUNK, CHUNK), CHUNK), :]
    listed = ice > 0.5
    load = jnp.zeros((CHUNK, COLS), jnp.float32)
    area_total = jnp.zeros((CHUNK, COLS), jnp.float32)
    air = air_ref[...]
    heat = heat_ref[...]
    for cat in range(CATS):
        temps = [temps_ref[cat * LAYERS + i] for i in range(LAYERS)]
        thick = thick_ref[cat]
        current, growth = column(temps, thick, snow_ref[cat], air)
        for i in range(LAYERS):
            temps_out[cat * LAYERS + i] = jnp.where(listed, current[i], temps[i])
        thick_new = jnp.where(listed, thick + (growth - 0.0005 * heat), thick)
        thick_out[cat] = thick_new
        area = area_ref[cat]
        load = load + area * thick_new
        area_total = area_total + area
    load = ice * load
    strength = load * jnp.exp(-20.0 * (1.0 - area_total))
    fields = [vel_ref[0], vel_ref[1], stress_ref[0], stress_ref[1], stress_ref[2]]
    forcing = [
        wind_ref[0] + ocean_ref[0],
        wind_ref[1] + ocean_ref[1],
        cells_ref[...].astype(jnp.float32),
        strength,
        0.9 * load,
    ]
    for i, x in enumerate(forcing):
        forcing_out[i] = x
    lane = lax.broadcasted_iota(jnp.int32, (CHUNK, 128), 1)
    group = lax.shift_right_logical(lane, 3)
    left = jnp.zeros((CHUNK, 128), jnp.float32)
    right = jnp.zeros((CHUNK, 128), jnp.float32)
    for i, x in enumerate(fields + forcing):
        first = x[:, :128]
        final = x[:, COLS - 128 :]
        if i:
            first = pltpu.roll(first, 8 * i, axis=1)
        final = pltpu.roll(final, (8 * i + 8) % 128, axis=1)
        left = jnp.where(group == i, first, left)
        right = jnp.where(group == i, final, right)
    left_out[...] = left
    right_out[...] = right


def halo_tile(west, east, field, rows):
    lane = lax.broadcasted_iota(jnp.int32, (rows, 128), 1)
    east_side = pltpu.roll(east, (128 - 8 * field) % 128, axis=1) if field else east
    west_side = pltpu.roll(west, (120 - 8 * field) % 128, axis=1)
    zero = jnp.zeros((rows, 128), jnp.float32)
    return jnp.where(lane < DEEP, east_side, jnp.where(lane >= 128 - DEEP, west_side, zero))


def rows_kernel(spot_ref, vel_ref, stress_ref, forcing_ref, west_ref, east_ref, even_out, odd_out):
    even = lax.rem(spot_ref[0], 2) == 0
    for side, start in ((0, 0), (1, ROWS - DEEP)):
        out = odd_out if side == 0 else even_out
        other = even_out if side == 0 else odd_out
        west = west_ref[start : start + DEEP, :]
        east = east_ref[start : start + DEEP, :]
        for i in range(FIELDS):
            ref, at = (vel_ref, i) if i < 2 else (stress_ref, i - 2) if i < 5 else (forcing_ref, i - 5)
            inner = ref[at, start : start + DEEP, :]
            tile = halo_tile(west, east, i, DEEP)

            @pl.when(even)
            def _():
                out[i, :, :COLS] = inner
                out[i, :, COLS:] = tile

            @pl.when(jnp.logical_not(even))
            def _():
                other[i, :, :COLS] = inner
                other[i, :, COLS:] = tile


def flip(x):
    lane = 127 - lax.broadcasted_iota(jnp.int32, (DEEP, 128), 1)
    turned = jnp.take_along_axis(x, lane, axis=1)
    return jnp.concatenate([turned[i : i + 1] for i in range(DEEP - 1, -1, -1)], axis=0)


def motion_kernel(
    spot_ref, vel_ref, stress_ref, forcing_ref, west_ref, east_ref, even_ref, odd_ref,
    vel_out, stress_out, state_ref,
):
    spot = spot_ref[0]
    even = lax.rem(spot, 2) == 0
    top = spot == spot_ref[1] - 1
    low = slice(DEEP, 2 * DEEP)
    mid = slice(2 * DEEP, 2 * DEEP + ROWS)
    high = slice(2 * DEEP + ROWS, 3 * DEEP + ROWS)
    for i in range(FIELDS):
        ref, at = (vel_ref, i) if i < 2 else (stress_ref, i - 2) if i < 5 else (forcing_ref, i - 5)
        state_ref[i, mid, :COLS] = ref[at]
        state_ref[i, mid, COLS:] = halo_tile(west_ref[...], east_ref[...], i, ROWS)
        state_ref[i, :DEEP, :] = jnp.zeros((DEEP, WIDE), jnp.float32)
        state_ref[i, TALL - DEEP :, :] = jnp.zeros((DEEP, WIDE), jnp.float32)

        @pl.when(even)
        def _():
            state_ref[i, high, :] = even_ref[i]
            state_ref[i, low, :] = odd_ref[i]

        @pl.when(jnp.logical_not(even))
        def _():
            state_ref[i, low, :] = even_ref[i]

            @pl.when(top)
            def _():
                sign = -1.0 if i in (0, 1, 5, 6) else 1.0
                for tile, source in ((0, 1), (1, 0), (2, 2)):
                    state_ref[i, high, tile * 128 : tile * 128 + 128] = sign * flip(
                        odd_ref[i, :, source * 128 : source * 128 + 128]
                    )

            @pl.when(jnp.logical_not(top))
            def _():
                state_ref[i, high, :] = odd_ref[i]

    bands = (TALL - 2 * DEEP) // BAND

    def prepare(band, carry):
        start = pl.multiple_of(DEEP + band * BAND, 8)
        at = pl.ds(start, BAND)
        row = lax.broadcasted_iota(jnp.int32, (BAND, 128), 0) + (start - 2 * DEEP) + spot * ROWS
        whole = spot_ref[1] * ROWS
        row = jnp.where(row >= whole, 2 * whole - 1 - row, row)
        latitude = row.astype(jnp.float32) + 0.5
        turn = 1.4 * jnp.sin(0.5 * jnp.pi * (2.0 * latitude / whole.astype(jnp.float32) - 1.0))
        turn = jnp.concatenate([turn] * 3, axis=1)
        mass = state_ref[9, at, :]
        diagonal = mass + 1.0
        turning = turn * mass
        scale = state_ref[7, at, :] / (diagonal * diagonal + turning * turning)
        state_ref[7, at, :] = diagonal * scale
        state_ref[10, at, :] = turning * scale
        return carry

    lax.fori_loop(0, bands, prepare, 0)

    def shift_x(x):
        return pltpu.roll(x, WIDE - 1, axis=1) - pltpu.roll(x, 1, axis=1)

    def tall(field, start):
        return state_ref[field, pl.ds(pl.multiple_of(start - 8, 8), BAND + 16), :]

    def shift_y(x):
        return x[9 : 9 + BAND] - x[7 : 7 + BAND]

    def stresses(band, carry):
        start = pl.multiple_of(DEEP + band * BAND, 8)
        at = pl.ds(start, BAND)
        east = tall(0, start)
        north = tall(1, start)
        east_dx = shift_x(east[8 : 8 + BAND])
        north_dx = shift_x(north[8 : 8 + BAND])
        east_dy = shift_y(east)
        north_dy = shift_y(north)
        diverge = 0.5 * (east_dx + north_dy)
        tension = 0.5 * (east_dx - north_dy)
        shearing = 0.5 * (east_dy + north_dx)
        deform = diverge * diverge + 0.25 * (tension * tension + shearing * shearing) + 1.0
        strength = state_ref[8, at, :]
        bulk = strength * lax.rsqrt(deform)
        state_ref[2, at, :] = state_ref[2, at, :] * (2.0 / 3.0) + (bulk * diverge - strength) * (1.0 / 3.0)
        state_ref[3, at, :] = state_ref[3, at, :] * (2.0 / 3.0) + bulk * tension * (1.0 / 12.0)
        state_ref[4, at, :] = state_ref[4, at, :] * (2.0 / 3.0) + bulk * shearing * (1.0 / 24.0)
        return carry

    def momentum(band, carry):
        start = pl.multiple_of(DEEP + band * BAND, 8)
        at = pl.ds(start, BAND)
        total = tall(2, start)
        differ = tall(3, start)
        shear = tall(4, start)
        normal_dx = shift_x(0.5 * (total[8 : 8 + BAND] + differ[8 : 8 + BAND]))
        shear_dx = shift_x(shear[8 : 8 + BAND])
        shear_dy = shift_y(shear)
        normal_dy = shift_y(0.5 * (total - differ))
        mass = state_ref[9, at, :]
        right_east = mass * state_ref[0, at, :] + 0.5 * (normal_dx + shear_dy) + state_ref[5, at, :]
        right_north = mass * state_ref[1, at, :] + 0.5 * (shear_dx + normal_dy) + state_ref[6, at, :]
        straight = state_ref[7, at, :]
        turned = state_ref[10, at, :]
        state_ref[0, at, :] = straight * right_east + turned * right_north
        state_ref[1, at, :] = straight * right_north - turned * right_east
        return carry

    def subcycle(turn, carry):
        lax.fori_loop(0, bands, stresses, 0)
        lax.fori_loop(0, bands, momentum, 0)
        return carry

    lax.fori_loop(0, SUB, subcycle, 0)
    for i in range(2):
        vel_out[i] = state_ref[i, mid, :COLS]
    for i in range(3):
        stress_out[i] = state_ref[2 + i, mid, :COLS]


def per_device(
    layer_temps, ice_thick, snow_thick, ice_area, air_temp, ocean_heat,
    velocity, stress, wind_stress, ocean_current, ocean_mask, ice_cols,
):
    stacked = CATS * LAYERS
    f32 = jnp.float32

    def rows3(n):
        return pl.BlockSpec((n, CHUNK, COLS), lambda i: (0, i, 0))

    rows2 = pl.BlockSpec((CHUNK, COLS), lambda i: (i, 0))
    edge = pl.BlockSpec((CHUNK, 128), lambda i: (i, 0))
    listed = ice_cols.reshape(1, -1)
    temps_new, thick_new, forcing, left, right = pl.pallas_call(
        thermo_kernel,
        name="thermo",
        grid=(ROWS // CHUNK,),
        in_specs=[
            pl.BlockSpec(listed.shape, lambda i: (0, 0)),
            rows3(stacked), rows3(CATS), rows3(CATS), rows3(CATS), rows2, rows2,
            rows3(2), rows3(3), rows3(2), rows3(2), rows2,
        ],
        out_specs=[rows3(stacked), rows3(CATS), rows3(5), edge, edge],
        out_shape=[
            jax.ShapeDtypeStruct((stacked, ROWS, COLS), f32),
            jax.ShapeDtypeStruct((CATS, ROWS, COLS), f32),
            jax.ShapeDtypeStruct((5, ROWS, COLS), f32),
            jax.ShapeDtypeStruct((ROWS, 128), f32),
            jax.ShapeDtypeStruct((ROWS, 128), f32),
        ],
        scratch_shapes=[pltpu.VMEM((ROWS, COLS), f32)],
    )(
        listed, layer_temps, ice_thick, snow_thick, ice_area, air_temp, ocean_heat,
        velocity, stress, wind_stress, ocean_current, ocean_mask,
    )
    n_bx = lax.axis_size("bx")
    n_by = lax.axis_size("by")
    west = lax.ppermute(right, "bx", [(q, (q + 1) % n_bx) for q in range(n_bx)])
    east = lax.ppermute(left, "bx", [((q + 1) % n_bx, q) for q in range(n_bx)])

    spot = jnp.stack([lax.axis_index("by"), jnp.int32(n_by)]).astype(jnp.int32)
    smem = pl.BlockSpec(memory_space=pltpu.SMEM)
    vmem = pl.BlockSpec(memory_space=pltpu.VMEM)
    band = jax.ShapeDtypeStruct((FIELDS, DEEP, WIDE), f32)
    even_rows, odd_rows = pl.pallas_call(
        rows_kernel,
        name="edge_rows",
        in_specs=[smem] + [vmem] * 5,
        out_specs=[vmem, vmem],
        out_shape=[band, band],
    )(spot, velocity, stress, forcing, west, east)

    def at(p, q):
        return q * n_by + p

    even_pairs, odd_pairs = [], []
    for q in range(n_bx):
        for p in range(0, n_by, 2):
            even_pairs += [(at(p, q), at(p + 1, q)), (at(p + 1, q), at(p, q))]
        for p in range(1, n_by - 1, 2):
            odd_pairs += [(at(p, q), at(p + 1, q)), (at(p + 1, q), at(p, q))]
        odd_pairs.append((at(n_by - 1, q), at(n_by - 1, n_bx - 1 - q)))
    even_halo = lax.ppermute(even_rows, ("bx", "by"), even_pairs)
    odd_halo = lax.ppermute(odd_rows, ("bx", "by"), odd_pairs)

    velocity_new, stress_new = pl.pallas_call(
        motion_kernel,
        name="motion",
        in_specs=[smem] + [vmem] * 7,
        out_specs=[vmem, vmem],
        out_shape=[
            jax.ShapeDtypeStruct((2, ROWS, COLS), f32),
            jax.ShapeDtypeStruct((3, ROWS, COLS), f32),
        ],
        scratch_shapes=[pltpu.VMEM((FIELDS + 1, TALL, WIDE), f32)],
    )(spot, velocity, stress, forcing, west, east, even_halo, odd_halo)
    return temps_new, thick_new, velocity_new, stress_new


def solution(mesh):
    grid3 = P(None, "by", "bx")
    grid2 = P("by", "bx")
    in_specs = (
        grid3, grid3, grid3, grid3, grid2, grid2, grid3, grid3, grid3, grid3, grid2,
        P("by", "bx", None),
    )
    return jax.shard_map(
        per_device, mesh=mesh, in_specs=in_specs, out_specs=(grid3,) * 4, check_vma=False
    )
```

```python
import jax
import jax.numpy as jnp
from jax import lax
from jax.experimental import pallas as pl
from jax.experimental.pallas import tpu as pltpu
from jax.sharding import PartitionSpec as P

ITERS = 4
SUB = 4
CATS = 5
LAYERS = 8
ROWS = 128
COLS = 256
DEEP = 8
FIELDS = 10
TALL = ROWS + 4 * DEEP
BAND = 24
LANES = 128
TILES = 32
FLAT = TILES * 8
STACKED = CATS * LAYERS
KEPT = STACKED + CATS
GROUPS = 8

FREEZING = -1.8
K_BASE = 2.03
K_GAIN = 0.47
K_SNOW = 0.31
ROOT = K_BASE / K_GAIN


def inverse(x):
    return 1.0 / x


def column(temps, thick, snow, air):
    depth = thick * (1.0 / (LAYERS - 1))
    square = depth * depth
    slope = square * (360.0 / K_GAIN)
    floor = square * (10.5 / K_GAIN)
    inv_depth = inverse(depth)
    snow_res = snow * inv_depth * (K_GAIN / K_SNOW)
    top_link = depth * (0.5 / K_GAIN) * inverse(snow * (0.5 / K_SNOW) + 0.05)
    snow_cap = snow * depth * (10.5 / K_GAIN)
    top_sum = snow_cap + top_link
    top_right = snow_cap * temps[0] + top_link * air
    current = list(temps)
    last = LAYERS - 1
    for repeat in range(ITERS):
        soft = [None] + [inverse(current[i] * current[i] + 1.0) for i in range(1, LAYERS)]
        conduct = [None] + [soft[i] + ROOT for i in range(1, LAYERS)]
        res = [snow_res] + [inverse(conduct[i]) for i in range(1, LAYERS)]
        cap = [None] + [slope * soft[i] + floor for i in range(1, LAYERS)]
        link = [res[i] + res[i + 1] for i in range(last)]
        ratio = [None] * LAYERS
        value = [None] * LAYERS
        down, down_flux = None, None
        for i in range(0, 4):
            total = top_sum if i == 0 else cap[i] + down
            right = top_right if i == 0 else cap[i] * temps[i] + down_flux
            ratio[i] = inverse(total * link[i] + 1.0)
            down = total * ratio[i]
            down_flux = right * ratio[i]
            value[i] = link[i] * down_flux
        up = conduct[last]
        up_flux = up * FREEZING
        for i in range(last, 4, -1):
            total = cap[i] + up
            right = cap[i] * temps[i] + up_flux
            ratio[i] = inverse(total * link[i - 1] + 1.0)
            up = total * ratio[i]
            up_flux = right * ratio[i]
            value[i] = link[i - 1] * up_flux
        renewed = [None] * LAYERS
        renewed[4] = (cap[4] * temps[4] + (down_flux + up_flux)) * inverse(cap[4] + (down + up))
        for i in range(3, -1, -1):
            if i > 0 or repeat == ITERS - 1:
                renewed[i] = value[i] + ratio[i] * renewed[i + 1]
        for i in range(5, LAYERS):
            renewed[i] = value[i] + ratio[i] * renewed[i - 1]
        current = renewed
    base = inverse(current[last] * current[last] + 1.0) + ROOT
    growth = (2.0 * K_GAIN * 0.0005) * (base * inv_depth) * (FREEZING - current[last])
    return current, growth


def draw_mask(list_ref):
    step = 512
    total = jnp.zeros((FLAT, LANES), jnp.float32)
    row_iota = lax.broadcasted_iota(jnp.int32, (FLAT, step), 0).astype(jnp.float32).astype(jnp.bfloat16)
    lane_iota = lax.broadcasted_iota(jnp.int32, (LANES, step), 0).astype(jnp.float32).astype(jnp.bfloat16)
    one = jnp.bfloat16(1.0)
    zero = jnp.bfloat16(0.0)
    for start in range(0, list_ref.shape[1], step):
        cells = list_ref[:, start : start + step]
        row = lax.shift_right_arithmetic(cells, 8) + (lax.bitwise_and(cells, 128))
        row = jnp.where(cells >= 0, row, -1).astype(jnp.float32).astype(jnp.bfloat16)
        lane = lax.bitwise_and(cells, 127).astype(jnp.float32).astype(jnp.bfloat16)
        total = total + lax.dot_general(
            jnp.where(row_iota == row, one, zero),
            jnp.where(lane_iota == lane, one, zero),
            (((1,), (1,)), ((), ())),
            preferred_element_type=jnp.float32,
        )
    return total


def index_cells(list_ref, mask_ref, base_ref, count_ref, inverse_ref, table_ref):
    mask = draw_mask(list_ref)
    mask_ref[...] = mask
    small = mask.astype(jnp.bfloat16)
    before = lax.broadcasted_iota(jnp.int32, (LANES, LANES), 0) < lax.broadcasted_iota(jnp.int32, (LANES, LANES), 1)
    before = before.astype(jnp.float32).astype(jnp.bfloat16)
    prefix = jnp.dot(small, before, preferred_element_type=jnp.float32).astype(jnp.int32)
    count = jnp.dot(small, jnp.ones((LANES, LANES), jnp.bfloat16), preferred_element_type=jnp.float32).astype(jnp.int32)
    count_ref[...] = count
    lane = lax.broadcasted_iota(jnp.int32, (8, LANES), 1)
    running = jnp.zeros((8, LANES), jnp.int32)
    bases = jnp.zeros((8, LANES), jnp.int32)
    ends = jnp.zeros((8, LANES), jnp.int32)
    for t in range(TILES):
        base_ref[8 * t : 8 * t + 8, :] = running
        bases = jnp.where(lane == t, running, bases)
        running = running + count[8 * t : 8 * t + 8]
        ends = jnp.where(lane == t, running, ends)
    wide_lane = lax.broadcasted_iota(jnp.int32, (FLAT, LANES), 1)
    moved = jnp.where(mask > 0.5, (wide_lane - prefix) * 256 + wide_lane, 0)
    for bit in range(7):
        probe = 256 << bit
        near = pltpu.roll(moved, LANES - (1 << bit), axis=1)
        moved = jnp.where(
            lax.bitwise_and(near, probe) != 0,
            near,
            jnp.where(lax.bitwise_and(moved, probe) != 0, 0, moved),
        )
    inverse_ref[...] = lax.bitwise_and(moved, 127)
    place = prefix + base_ref[...]
    base_min = jnp.min(bases, axis=0, keepdims=True)
    end_max = jnp.max(ends, axis=0, keepdims=True)
    used = lax.broadcasted_iota(jnp.int32, (TILES, LANES), 1) < TILES
    level = lax.broadcasted_iota(jnp.int32, (TILES, LANES), 0) * LANES
    first = jnp.sum(jnp.where(jnp.logical_and(used, end_max <= level), 1.0, 0.0), axis=1, keepdims=True)
    final = jnp.sum(jnp.where(jnp.logical_and(used, base_min < level + LANES), 1.0, 0.0), axis=1, keepdims=True)
    spread = lax.broadcasted_iota(jnp.int32, (TILES, LANES), 1)
    table_ref[:TILES, :] = jnp.where(spread == 0, first, final).astype(jnp.int32)
    top = lax.broadcasted_iota(jnp.int32, (8, LANES), 0)
    table_ref[TILES:, :] = jnp.where(top == 0, base_min, end_max)
    return place


def thermo_kernel(
    list_ref, temps_hbm, thick_hbm, snow_hbm, area_hbm, air_hbm, heat_hbm,
    vel_hbm, stress_hbm, wind_hbm, ocean_hbm, cells_hbm,
    temps_out, thick_out, forcing_out, left_out, right_out,
    kept_ref, snow_ref, area_ref, single_ref, moving_ref, drive_ref, cells_ref, forcing_ref,
    mask_ref, base_ref, count_ref, inverse_ref, place_ref, table_ref, gathered_ref, result_ref,
    plan_ref, in_sem, out_sem, table_sem,
):
    halves = ((0, slice(0, LANES), slice(0, ROWS)), (1, slice(LANES, COLS), slice(ROWS, FLAT)))
    copies = []
    order = 0
    for source, target in (
        (temps_hbm, kept_ref.at[:STACKED]),
        (thick_hbm, kept_ref.at[STACKED:]),
        (snow_hbm, snow_ref),
        (air_hbm, single_ref.at[0]),
        (heat_hbm, single_ref.at[1]),
        (area_hbm, area_ref),
        (vel_hbm, moving_ref.at[0:2]),
        (stress_hbm, moving_ref.at[2:5]),
        (wind_hbm, drive_ref.at[0:2]),
        (ocean_hbm, drive_ref.at[2:4]),
        (cells_hbm, cells_ref),
    ):
        for half, span, rows in halves:
            if len(source.shape) == 3:
                copy = pltpu.make_async_copy(source.at[:, :, span], target.at[:, rows, :], in_sem.at[order])
            else:
                copy = pltpu.make_async_copy(source.at[:, span], target.at[rows, :], in_sem.at[order])
            copy.start()
            copies.append(copy)
            order += 1

    place_ref[...] = index_cells(list_ref, mask_ref, base_ref, count_ref, inverse_ref, table_ref)
    plan = pltpu.make_async_copy(table_ref, plan_ref, table_sem)
    plan.start()
    for copy in copies:
        copy.wait()
    plan.wait()
    lane = lax.broadcasted_iota(jnp.int32, (8, LANES), 1)

    def solve(level, carry):
        begin = plan_ref[level, 0]
        end = plan_ref[level, 1]

        def gather(turn, inner):
            picks = []
            for offset in range(4):
                tile = jnp.minimum(begin + turn * 4 + offset, TILES - 1)
                at = pl.ds(pl.multiple_of(tile * 8, 8), 8)
                rank = lane + level * LANES - base_ref[at, :]
                inside = jnp.logical_and(rank >= 0, rank < count_ref[at, :])
                rank = jnp.where(inside, rank, 0)
                spot = jnp.take_along_axis(inverse_ref[at, :], rank, axis=1)
                picks.append((at, inside, spot))
            planes = [(kept_ref, p) for p in range(KEPT)]
            planes += [(snow_ref, p) for p in range(CATS)] + [(single_ref, 0), (single_ref, 1)]
            for number, (ref, p) in enumerate(planes):
                value = gathered_ref[number]
                for at, inside, spot in picks:
                    value = jnp.where(inside, jnp.take_along_axis(ref[p, at, :], spot, axis=1), value)
                gathered_ref[number] = value
            return inner

        lax.fori_loop(0, lax.div(end - begin + 3, 4), gather, 0)
        air = gathered_ref[KEPT + CATS]
        heat = gathered_ref[KEPT + CATS + 1]
        for cat in range(CATS):
            temps = [gathered_ref[cat * LAYERS + i] for i in range(LAYERS)]
            thick = gathered_ref[STACKED + cat]
            current, growth = column(temps, thick, gathered_ref[KEPT + cat], air)
            for i in range(LAYERS):
                result_ref[level, cat * LAYERS + i] = current[i]
            result_ref[level, STACKED + cat] = thick + (growth - 0.0005 * heat)
        return carry

    levels = lax.div(plan_ref[TILES + 1, TILES - 1] + (LANES - 1), LANES)
    lax.fori_loop(0, levels, solve, 0)

    def spread(tile, carry):
        at = pl.ds(pl.multiple_of(tile * 8, 8), 8)
        first = lax.div(plan_ref[TILES, tile], LANES)
        final = lax.div(plan_ref[TILES + 1, tile] + (LANES - 1), LANES)
        place = place_ref[at, :]
        ice = mask_ref[at, :]
        level = jnp.where(ice > 0.5, lax.shift_right_logical(place, 7), -1)
        spot = lax.bitwise_and(place, LANES - 1)

        def fill(turn, inner):
            low = jnp.minimum(first + 2 * turn, TILES - 1)
            high = jnp.minimum(low + 1, TILES - 1)
            in_low = level == low
            in_high = level == high
            for p in range(KEPT):
                from_low = jnp.take_along_axis(result_ref[low, p], spot, axis=1)
                from_high = jnp.take_along_axis(result_ref[high, p], spot, axis=1)
                kept_ref[p, at, :] = jnp.where(in_low, from_low, jnp.where(in_high, from_high, kept_ref[p, at, :]))
            return inner

        lax.fori_loop(0, lax.div(final - first + 1, 2), fill, 0)
        load = jnp.zeros((8, LANES), jnp.float32)
        area_total = jnp.zeros((8, LANES), jnp.float32)
        for cat in range(CATS):
            area = area_ref[cat, at, :]
            load = load + area * kept_ref[STACKED + cat, at, :]
            area_total = area_total + area
        load = ice * load
        forcing_ref[0, at, :] = drive_ref[0, at, :] + drive_ref[2, at, :]
        forcing_ref[1, at, :] = drive_ref[1, at, :] + drive_ref[3, at, :]
        forcing_ref[2, at, :] = cells_ref[at, :].astype(jnp.float32)
        forcing_ref[3, at, :] = load * jnp.exp(-20.0 * (1.0 - area_total))
        forcing_ref[4, at, :] = 0.9 * load
        return carry

    def send_out(group):
        pieces = []
        per_half = GROUPS // 2
        height = ROWS // per_half
        half, inner = group // per_half, group % per_half
        span = slice(half * LANES, half * LANES + LANES)
        there = slice(inner * height, inner * height + height)
        here = slice(group * height, group * height + height)
        pieces.append(pltpu.make_async_copy(
            kept_ref.at[:STACKED, here, :], temps_out.at[:, there, span], out_sem.at[group, 0]))
        pieces.append(pltpu.make_async_copy(
            kept_ref.at[STACKED:, here, :], thick_out.at[:, there, span], out_sem.at[group, 1]))
        pieces.append(pltpu.make_async_copy(
            forcing_ref.at[:, here, :], forcing_out.at[:, there, span], out_sem.at[group, 2]))
        return pieces

    sent = []
    per_group = TILES // GROUPS
    for group in range(GROUPS):
        lax.fori_loop(group * per_group, group * per_group + per_group, spread, 0)
        for copy in send_out(group):
            copy.start()
            sent.append(copy)

    def pack(tile, carry):
        group = lax.shift_right_logical(lane, 3)
        for out_ref, half, push in ((left_out, 0, 0), (right_out, 1, 8)):
            at = pl.ds(pl.multiple_of(tile * 8 + half * ROWS, 8), 8)
            packed = jnp.zeros((8, LANES), jnp.float32)
            for i in range(FIELDS):
                x = moving_ref[i, at, :] if i < 5 else forcing_ref[i - 5, at, :]
                turn = (8 * i + push) % LANES
                if turn:
                    x = pltpu.roll(x, turn, axis=1)
                packed = jnp.where(group == i, x, packed)
            out_ref[pl.ds(pl.multiple_of(tile * 8, 8), 8), :] = packed
        return carry

    lax.fori_loop(0, ROWS // 8, pack, 0)
    for copy in sent:
        copy.wait()


def halo_tile(west, east, field, rows):
    lane = lax.broadcasted_iota(jnp.int32, (rows, LANES), 1)
    east_side = pltpu.roll(east, (LANES - 8 * field) % LANES, axis=1) if field else east
    west_side = pltpu.roll(west, (120 - 8 * field) % LANES, axis=1)
    zero = jnp.zeros((rows, LANES), jnp.float32)
    return jnp.where(lane < DEEP, east_side, jnp.where(lane >= LANES - DEEP, west_side, zero))


def rows_kernel(
    spot_ref, vel_low, stress_low, forcing_low, west_low, east_low,
    vel_high, stress_high, forcing_high, west_high, east_high, even_out, odd_out,
):
    even = lax.rem(spot_ref[0], 2) == 0

    def fill(to_low, to_high):
        for out, vel_ref, stress_ref, forcing_ref, west_ref, east_ref in (
            (to_low, vel_low, stress_low, forcing_low, west_low, east_low),
            (to_high, vel_high, stress_high, forcing_high, west_high, east_high),
        ):
            for i in range(FIELDS):
                ref, at = (vel_ref, i) if i < 2 else (stress_ref, i - 2) if i < 5 else (forcing_ref, i - 5)
                out[i, 0] = ref[at, :, :LANES]
                out[i, 1] = ref[at, :, LANES:]
                out[i, 2] = halo_tile(west_ref[...], east_ref[...], i, DEEP)

    @pl.when(even)
    def _():
        fill(odd_out, even_out)

    @pl.when(jnp.logical_not(even))
    def _():
        fill(even_out, odd_out)


def flip(x):
    lane = (LANES - 1) - lax.broadcasted_iota(jnp.int32, (DEEP, LANES), 1)
    turned = jnp.take_along_axis(x, lane, axis=1)
    return jnp.concatenate([turned[i : i + 1] for i in range(DEEP - 1, -1, -1)], axis=0)


def motion_kernel(
    spot_ref, vel_hbm, stress_hbm, forcing_hbm, west_ref, east_ref, even_ref, odd_ref,
    vel_out, stress_out, state_ref, in_sem, out_sem,
):
    spot = spot_ref[0]
    even = lax.rem(spot, 2) == 0
    top = spot == spot_ref[1] - 1
    low = slice(DEEP, 2 * DEEP)
    mid = slice(2 * DEEP, 2 * DEEP + ROWS)
    high = slice(2 * DEEP + ROWS, 3 * DEEP + ROWS)
    copies = []
    for tile in range(2):
        span = slice(tile * LANES, tile * LANES + LANES)
        for number, (source, target) in enumerate((
            (vel_hbm, state_ref.at[0:2, tile, mid, :]),
            (stress_hbm, state_ref.at[2:5, tile, mid, :]),
            (forcing_hbm, state_ref.at[5:10, tile, mid, :]),
        )):
            copy = pltpu.make_async_copy(source.at[:, :, span], target, in_sem.at[tile, number])
            copy.start()
            copies.append(copy)
    blank = jnp.zeros((DEEP, LANES), jnp.float32)
    for i in range(FIELDS):
        for tile in range(3):
            state_ref[i, tile, :DEEP, :] = blank
            state_ref[i, tile, TALL - DEEP :, :] = blank
        state_ref[i, 2, mid, :] = halo_tile(west_ref[...], east_ref[...], i, ROWS)

    @pl.when(even)
    def _():
        for i in range(FIELDS):
            for tile in range(3):
                state_ref[i, tile, high, :] = even_ref[i, tile]
                state_ref[i, tile, low, :] = odd_ref[i, tile]

    @pl.when(jnp.logical_not(even))
    def _():
        for i in range(FIELDS):
            for tile in range(3):
                state_ref[i, tile, low, :] = even_ref[i, tile]
                state_ref[i, tile, high, :] = odd_ref[i, tile]

    @pl.when(top)
    def _():
        for i in range(FIELDS):
            for tile, source in ((0, 1), (1, 0), (2, 2)):
                turned = flip(odd_ref[i, source])
                state_ref[i, tile, high, :] = -turned if i in (0, 1, 5, 6) else turned

    for copy in copies:
        copy.wait()
    bands = (TALL - 2 * DEEP) // BAND
    lane = lax.broadcasted_iota(jnp.int32, (BAND, LANES), 1)
    is_first = lane == 0
    is_final = lane == LANES - 1

    def prepare(band, carry):
        start = pl.multiple_of(DEEP + band * BAND, 8)
        at = pl.ds(start, BAND)
        row = lax.broadcasted_iota(jnp.int32, (BAND, LANES), 0) + (start - 2 * DEEP) + spot * ROWS
        whole = spot_ref[1] * ROWS
        row = jnp.where(row >= whole, 2 * whole - 1 - row, row)
        latitude = row.astype(jnp.float32) + 0.5
        turn = 1.4 * jnp.sin(0.5 * jnp.pi * (2.0 * latitude / whole.astype(jnp.float32) - 1.0))
        for tile in range(3):
            mass = state_ref[9, tile, at, :]
            diagonal = mass + 1.0
            turning = turn * mass
            scale = state_ref[7, tile, at, :] / (diagonal * diagonal + turning * turning)
            state_ref[7, tile, at, :] = diagonal * scale
            state_ref[10, tile, at, :] = turning * scale
        return carry

    lax.fori_loop(0, bands, prepare, 0)

    def shift_x(parts):
        ahead = [pltpu.roll(x, LANES - 1, axis=1) for x in parts]
        behind = [pltpu.roll(x, 1, axis=1) for x in parts]
        return [
            jnp.where(is_final, ahead[(k + 1) % 3], ahead[k]) - jnp.where(is_first, behind[(k + 2) % 3], behind[k])
            for k in range(3)
        ]

    def shift_y(field, tile, start):
        return state_ref[field, tile, pl.ds(start + 1, BAND), :] - state_ref[field, tile, pl.ds(start - 1, BAND), :]

    def stresses(band, carry):
        start = pl.multiple_of(DEEP + band * BAND, 8)
        at = pl.ds(start, BAND)
        east_dx = shift_x([state_ref[0, k, at, :] for k in range(3)])
        north_dx = shift_x([state_ref[1, k, at, :] for k in range(3)])
        for k in range(3):
            north_dy = shift_y(1, k, start)
            diverge = 0.5 * (east_dx[k] + north_dy)
            tension = 0.5 * (east_dx[k] - north_dy)
            shearing = 0.5 * (shift_y(0, k, start) + north_dx[k])
            deform = diverge * diverge + 0.25 * (tension * tension + shearing * shearing) + 1.0
            strength = state_ref[8, k, at, :] * (1.0 / 3.0)
            bulk = strength * lax.rsqrt(deform)
            viscous = bulk * 0.25
            state_ref[2, k, at, :] = state_ref[2, k, at, :] * (2.0 / 3.0) + (bulk * diverge - strength)
            state_ref[3, k, at, :] = state_ref[3, k, at, :] * (2.0 / 3.0) + viscous * tension
            state_ref[4, k, at, :] = state_ref[4, k, at, :] * (2.0 / 3.0) + viscous * (0.5 * shearing)
        return carry

    def momentum(band, carry):
        start = pl.multiple_of(DEEP + band * BAND, 8)
        at = pl.ds(start, BAND)
        up = pl.ds(start + 1, BAND)
        down = pl.ds(start - 1, BAND)
        normal_dx = shift_x([state_ref[2, k, at, :] + state_ref[3, k, at, :] for k in range(3)])
        shear_dx = shift_x([state_ref[4, k, at, :] for k in range(3)])
        for k in range(3):
            shear_dy = shift_y(4, k, start)
            normal_dy = (state_ref[2, k, up, :] - state_ref[3, k, up, :]) - (
                state_ref[2, k, down, :] - state_ref[3, k, down, :]
            )
            mass = state_ref[9, k, at, :]
            right_east = mass * state_ref[0, k, at, :] + (0.25 * normal_dx[k] + 0.5 * shear_dy) + state_ref[5, k, at, :]
            right_north = mass * state_ref[1, k, at, :] + (0.5 * shear_dx[k] + 0.25 * normal_dy) + state_ref[6, k, at, :]
            straight = state_ref[7, k, at, :]
            turned = state_ref[10, k, at, :]
            state_ref[0, k, at, :] = straight * right_east + turned * right_north
            state_ref[1, k, at, :] = straight * right_north - turned * right_east
        return carry

    def subcycle(turn, carry):
        lax.fori_loop(0, bands, stresses, 0)
        lax.fori_loop(0, bands, momentum, 0)
        return carry

    lax.fori_loop(0, SUB, subcycle, 0)
    sent = []
    for tile in range(2):
        span = slice(tile * LANES, tile * LANES + LANES)
        for number, (source, target) in enumerate((
            (state_ref.at[0:2, tile, mid, :], vel_out),
            (state_ref.at[2:5, tile, mid, :], stress_out),
        )):
            copy = pltpu.make_async_copy(source, target.at[:, :, span], out_sem.at[tile, number])
            copy.start()
            sent.append(copy)
    for copy in sent:
        copy.wait()


def per_device(
    layer_temps, ice_thick, snow_thick, ice_area, air_temp, ocean_heat,
    velocity, stress, wind_stress, ocean_current, ocean_mask, ice_cols,
):
    f32 = jnp.float32
    i32 = jnp.int32
    smem = pl.BlockSpec(memory_space=pltpu.SMEM)
    vmem = pl.BlockSpec(memory_space=pltpu.VMEM)
    here = pl.BlockSpec(memory_space=pl.ANY)
    listed = ice_cols.reshape(1, -1)

    def flat(n, kind=f32):
        return pltpu.VMEM((n, FLAT, LANES), kind)

    one = pltpu.VMEM((FLAT, LANES), i32)
    temps_new, thick_new, forcing, left, right = pl.pallas_call(
        thermo_kernel,
        name="thermo",
        in_specs=[vmem] + [here] * 11,
        out_specs=[here, here, here, vmem, vmem],
        out_shape=[
            jax.ShapeDtypeStruct((STACKED, ROWS, COLS), f32),
            jax.ShapeDtypeStruct((CATS, ROWS, COLS), f32),
            jax.ShapeDtypeStruct((5, ROWS, COLS), f32),
            jax.ShapeDtypeStruct((ROWS, LANES), f32),
            jax.ShapeDtypeStruct((ROWS, LANES), f32),
        ],
        scratch_shapes=[
            flat(KEPT), flat(CATS), flat(CATS), flat(2), flat(5), flat(4), one, flat(5),
            pltpu.VMEM((FLAT, LANES), f32), one, one, one, one,
            pltpu.VMEM((TILES + 8, LANES), i32),
            pltpu.VMEM((KEPT + CATS + 2, 8, LANES), f32),
            pltpu.VMEM((TILES, KEPT, 8, LANES), f32),
            pltpu.SMEM((TILES + 8, LANES), i32),
            pltpu.SemaphoreType.DMA((22,)),
            pltpu.SemaphoreType.DMA((GROUPS, 3)),
            pltpu.SemaphoreType.DMA,
        ],
    )(
        listed, layer_temps, ice_thick, snow_thick, ice_area, air_temp, ocean_heat,
        velocity, stress, wind_stress, ocean_current, ocean_mask,
    )
    n_bx = lax.axis_size("bx")
    n_by = lax.axis_size("by")
    west = lax.ppermute(right, "bx", [(q, (q + 1) % n_bx) for q in range(n_bx)])
    east = lax.ppermute(left, "bx", [((q + 1) % n_bx, q) for q in range(n_bx)])

    spot = jnp.stack([lax.axis_index("by"), jnp.int32(n_by)]).astype(i32)
    band = jax.ShapeDtypeStruct((FIELDS, 3, DEEP, LANES), f32)

    def slab(n, block):
        return pl.BlockSpec((n, DEEP, COLS), lambda i: (0, block, 0))

    def edge(block):
        return pl.BlockSpec((DEEP, LANES), lambda i: (block, 0))

    final = ROWS // DEEP - 1
    halo = pl.BlockSpec((FIELDS, 3, DEEP, LANES), lambda i: (0, 0, 0, 0))
    even_rows, odd_rows = pl.pallas_call(
        rows_kernel,
        name="edge_rows",
        grid=(1,),
        in_specs=[smem]
        + [slab(2, 0), slab(3, 0), slab(5, 0), edge(0), edge(0)]
        + [slab(2, final), slab(3, final), slab(5, final), edge(final), edge(final)],
        out_specs=[halo, halo],
        out_shape=[band, band],
    )(spot, velocity, stress, forcing, west, east, velocity, stress, forcing, west, east)

    def at(p, q):
        return q * n_by + p

    even_pairs, odd_pairs = [], []
    for q in range(n_bx):
        for p in range(0, n_by, 2):
            even_pairs += [(at(p, q), at(p + 1, q)), (at(p + 1, q), at(p, q))]
        for p in range(1, n_by - 1, 2):
            odd_pairs += [(at(p, q), at(p + 1, q)), (at(p + 1, q), at(p, q))]
        odd_pairs.append((at(n_by - 1, q), at(n_by - 1, n_bx - 1 - q)))
    even_halo = lax.ppermute(even_rows, ("bx", "by"), even_pairs)
    odd_halo = lax.ppermute(odd_rows, ("bx", "by"), odd_pairs)

    velocity_new, stress_new = pl.pallas_call(
        motion_kernel,
        name="motion",
        in_specs=[smem] + [here] * 3 + [vmem] * 4,
        out_specs=[here, here],
        out_shape=[
            jax.ShapeDtypeStruct((2, ROWS, COLS), f32),
            jax.ShapeDtypeStruct((3, ROWS, COLS), f32),
        ],
        scratch_shapes=[
            pltpu.VMEM((FIELDS + 1, 3, TALL, LANES), f32),
            pltpu.SemaphoreType.DMA((2, 3)),
            pltpu.SemaphoreType.DMA((2, 2)),
        ],
    )(spot, velocity, stress, forcing, west, east, even_halo, odd_halo)
    return temps_new, thick_new, velocity_new, stress_new


def solution(mesh):
    grid3 = P(None, "by", "bx")
    grid2 = P("by", "bx")
    in_specs = (
        grid3, grid3, grid3, grid3, grid2, grid2, grid3, grid3, grid3, grid3, grid2,
        P("by", "bx", None),
    )
    return jax.shard_map(
        per_device, mesh=mesh, in_specs=in_specs, out_specs=(grid3,) * 4, check_vma=False
    )
```

```python
import jax
import jax.numpy as jnp
from jax import lax
from jax.experimental import pallas as pl
from jax.experimental.pallas import tpu as pltpu
from jax.sharding import PartitionSpec as P

ITERS = 4
SUB = 4
CATS = 5
LAYERS = 8
ROWS = 128
COLS = 256
DEEP = 8
FIELDS = 10
TALL = ROWS + 4 * DEEP
BAND = 144
LANES = 128
TILES = 32
FLAT = TILES * 8
STACKED = CATS * LAYERS
KEPT = STACKED + CATS
TEAM = 4
PAIR = 2
TURNS = TILES // (TEAM * PAIR)
HEIGHT = FLAT // TURNS
BLOCK = 13

FREEZING = -1.8
K_BASE = 2.03
K_GAIN = 0.47
K_SNOW = 0.31
ROOT = K_BASE / K_GAIN


def inverse(x):
    return 1.0 / x


def column(temps, thick, snow, air):
    depth = thick * (1.0 / (LAYERS - 1))
    square = depth * depth
    slope = square * (360.0 / K_GAIN)
    floor = square * (10.5 / K_GAIN)
    inv_depth = inverse(depth)
    snow_res = snow * inv_depth * (K_GAIN / K_SNOW)
    top_link = depth * (0.5 / K_GAIN) * inverse(snow * (0.5 / K_SNOW) + 0.05)
    snow_cap = snow * depth * (10.5 / K_GAIN)
    top_sum = snow_cap + top_link
    top_right = snow_cap * temps[0] + top_link * air
    current = list(temps)
    last = LAYERS - 1
    for repeat in range(ITERS):
        soft = [None] + [inverse(current[i] * current[i] + 1.0) for i in range(1, LAYERS)]
        conduct = [None] + [soft[i] + ROOT for i in range(1, LAYERS)]
        res = [snow_res] + [inverse(conduct[i]) for i in range(1, LAYERS)]
        cap = [None] + [slope * soft[i] + floor for i in range(1, LAYERS)]
        link = [res[i] + res[i + 1] for i in range(last)]
        ratio = [None] * LAYERS
        value = [None] * LAYERS
        down, down_flux = None, None
        for i in range(0, 4):
            total = top_sum if i == 0 else cap[i] + down
            right = top_right if i == 0 else cap[i] * temps[i] + down_flux
            ratio[i] = inverse(total * link[i] + 1.0)
            down = total * ratio[i]
            down_flux = right * ratio[i]
            value[i] = link[i] * down_flux
        up = conduct[last]
        up_flux = up * FREEZING
        for i in range(last, 4, -1):
            total = cap[i] + up
            right = cap[i] * temps[i] + up_flux
            ratio[i] = inverse(total * link[i - 1] + 1.0)
            up = total * ratio[i]
            up_flux = right * ratio[i]
            value[i] = link[i - 1] * up_flux
        renewed = [None] * LAYERS
        renewed[4] = (cap[4] * temps[4] + (down_flux + up_flux)) * inverse(cap[4] + (down + up))
        for i in range(3, -1, -1):
            if i > 0 or repeat == ITERS - 1:
                renewed[i] = value[i] + ratio[i] * renewed[i + 1]
        for i in range(5, LAYERS):
            renewed[i] = value[i] + ratio[i] * renewed[i - 1]
        current = renewed
    base = inverse(current[last] * current[last] + 1.0) + ROOT
    growth = (2.0 * K_GAIN * 0.0005) * (base * inv_depth) * (FREEZING - current[last])
    return current, growth


def draw_mask(list_ref):
    step = 512
    total = jnp.zeros((FLAT, LANES), jnp.float32)
    row_iota = lax.broadcasted_iota(jnp.int32, (FLAT, step), 0).astype(jnp.float32).astype(jnp.bfloat16)
    lane_iota = lax.broadcasted_iota(jnp.int32, (LANES, step), 0).astype(jnp.float32).astype(jnp.bfloat16)
    one = jnp.bfloat16(1.0)
    zero = jnp.bfloat16(0.0)
    for start in range(0, list_ref.shape[1], step):
        cells = list_ref[:, start : start + step]
        row = lax.shift_right_arithmetic(cells, 8) + (lax.bitwise_and(cells, 128))
        row = jnp.where(cells >= 0, row, -1).astype(jnp.float32).astype(jnp.bfloat16)
        lane = lax.bitwise_and(cells, 127).astype(jnp.float32).astype(jnp.bfloat16)
        total = total + lax.dot_general(
            jnp.where(row_iota == row, one, zero),
            jnp.where(lane_iota == lane, one, zero),
            (((1,), (1,)), ((), ())),
            preferred_element_type=jnp.float32,
        )
    return total


def index_cells(list_ref, mask_ref, base_ref, count_ref, inverse_ref, place_ref, spot_ref):
    mask = draw_mask(list_ref)
    mask_ref[...] = mask
    small = mask.astype(jnp.bfloat16)
    before = lax.broadcasted_iota(jnp.int32, (LANES, LANES), 0) < lax.broadcasted_iota(jnp.int32, (LANES, LANES), 1)
    before = before.astype(jnp.float32).astype(jnp.bfloat16)
    prefix = jnp.dot(small, before, preferred_element_type=jnp.float32).astype(jnp.int32)
    count = jnp.dot(small, jnp.ones((LANES, LANES), jnp.bfloat16), preferred_element_type=jnp.float32).astype(jnp.int32)
    count_ref[...] = count
    most = jnp.zeros((8, LANES), jnp.int32)
    running = most
    for t in range(TILES):
        if t % TEAM == 0:
            running = jnp.zeros((8, LANES), jnp.int32)
        base_ref[8 * t : 8 * t + 8, :] = running
        running = running + count[8 * t : 8 * t + 8]
        most = jnp.maximum(most, running)
    wide_lane = lax.broadcasted_iota(jnp.int32, (FLAT, LANES), 1)
    moved = jnp.where(mask > 0.5, (wide_lane - prefix) * 256 + wide_lane, 0)
    for bit in range(7):
        probe = 256 << bit
        near = pltpu.roll(moved, LANES - (1 << bit), axis=1)
        moved = jnp.where(
            lax.bitwise_and(near, probe) != 0,
            near,
            jnp.where(lax.bitwise_and(moved, probe) != 0, 0, moved),
        )
    inverse = lax.bitwise_and(moved, LANES - 1)
    inverse_ref[...] = inverse
    base = base_ref[...]
    place_ref[...] = jnp.where(mask > 0.5, prefix + base, -1)
    lane = lax.broadcasted_iota(jnp.int32, (8, LANES), 1)
    for t in range(TILES):
        here = slice(8 * t, 8 * t + 8)
        rank = lane - base_ref[here, :]
        inside = jnp.logical_and(rank >= 0, rank < count[here])
        spot = jnp.take_along_axis(inverse[here], jnp.where(inside, rank, 0), axis=1)
        spot_ref[here, :] = jnp.where(inside, spot, -1)
    return jnp.max(most)


def gather_team(picks, kept_ref, snow_ref, single_ref, gathered_ref):
    planes = [(kept_ref, p) for p in range(KEPT)]
    planes += [(snow_ref, p) for p in range(CATS)] + [(single_ref, 0), (single_ref, 1)]
    for start in range(0, len(planes), BLOCK):
        block = planes[start : start + BLOCK]
        values = [None] * len(block)
        for at, spot in picks:
            inside = spot >= 0
            spot = jnp.maximum(spot, 0)
            for k, (ref, p) in enumerate(block):
                value = jnp.take_along_axis(ref[p, at, :], spot, axis=1)
                values[k] = value if values[k] is None else jnp.where(inside, value, values[k])
        for k, value in enumerate(values):
            gathered_ref[start + k] = value


def solve_team(gathered_ref, result_ref):
    air = gathered_ref[KEPT + CATS]
    heat = gathered_ref[KEPT + CATS + 1]
    for cat in range(CATS):
        temps = [gathered_ref[cat * LAYERS + i] for i in range(LAYERS)]
        thick = gathered_ref[STACKED + cat]
        current, growth = column(temps, thick, gathered_ref[KEPT + cat], air)
        for i in range(LAYERS):
            result_ref[cat * LAYERS + i] = current[i]
        result_ref[STACKED + cat] = thick + (growth - 0.0005 * heat)


def spread_team(tiles, level, place_ref, source_ref, result_ref, fresh_ref):
    for at in tiles:
        place = place_ref[at, :] - level * LANES
        inside = jnp.logical_and(place >= 0, place < LANES)
        spot = jnp.where(inside, place, 0)
        for p in range(KEPT):
            value = jnp.take_along_axis(result_ref[p], spot, axis=1)
            fresh_ref[p, at, :] = jnp.where(inside, value, source_ref[p, at, :])


def thermo_kernel(
    list_ref, temps_hbm, thick_hbm, snow_hbm, area_hbm, air_hbm, heat_hbm,
    vel_hbm, stress_hbm, wind_hbm, ocean_hbm, cells_hbm,
    temps_out, thick_out, forcing_out, left_out, right_out,
    kept_ref, fresh_ref, snow_ref, area_ref, single_ref, moving_ref, drive_ref, cells_ref, forcing_ref,
    mask_ref, base_ref, count_ref, inverse_ref, place_ref, spot_ref,
    gathered_a, gathered_b, result_a, result_b, in_sem, out_sem,
):
    def fetch(turn):
        half, inner = turn // (TURNS // 2), turn % (TURNS // 2)
        span = slice(half * LANES, half * LANES + LANES)
        there = slice(inner * HEIGHT, inner * HEIGHT + HEIGHT)
        rows = slice(turn * HEIGHT, turn * HEIGHT + HEIGHT)
        copies = []
        for source, target in (
            (temps_hbm, kept_ref.at[:STACKED]),
            (thick_hbm, kept_ref.at[STACKED:]),
            (snow_hbm, snow_ref),
            (air_hbm, single_ref.at[0]),
            (heat_hbm, single_ref.at[1]),
            (area_hbm, area_ref),
            (wind_hbm, drive_ref.at[0:2]),
            (ocean_hbm, drive_ref.at[2:4]),
            (cells_hbm, cells_ref),
            (vel_hbm, moving_ref.at[0:2]),
            (stress_hbm, moving_ref.at[2:5]),
        ):
            sem = in_sem.at[turn, len(copies)]
            if len(source.shape) == 3:
                copies.append(pltpu.make_async_copy(source.at[:, there, span], target.at[:, rows, :], sem))
            else:
                copies.append(pltpu.make_async_copy(source.at[there, span], target.at[rows, :], sem))
        return copies

    def send(turn):
        half, inner = turn // (TURNS // 2), turn % (TURNS // 2)
        span = slice(half * LANES, half * LANES + LANES)
        there = slice(inner * HEIGHT, inner * HEIGHT + HEIGHT)
        rows = slice(turn * HEIGHT, turn * HEIGHT + HEIGHT)
        return [
            pltpu.make_async_copy(fresh_ref.at[:STACKED, rows, :], temps_out.at[:, there, span], out_sem.at[turn, 0]),
            pltpu.make_async_copy(fresh_ref.at[STACKED:, rows, :], thick_out.at[:, there, span], out_sem.at[turn, 1]),
            pltpu.make_async_copy(forcing_ref.at[:, rows, :], forcing_out.at[:, there, span], out_sem.at[turn, 2]),
        ]

    fetched = [fetch(turn) for turn in range(TURNS)]
    for copies in fetched:
        for copy in copies:
            copy.start()
    most = index_cells(list_ref, mask_ref, base_ref, count_ref, inverse_ref, place_ref, spot_ref)
    lane = lax.broadcasted_iota(jnp.int32, (8, LANES), 1)
    buffers = ((gathered_a, result_a), (gathered_b, result_b))

    def tiles_of(team):
        return [pl.ds(pl.multiple_of((team * TEAM + u) * 8, 8), 8) for u in range(TEAM)]

    def force(at):
        ice = mask_ref[at, :]
        load = jnp.zeros(ice.shape, jnp.float32)
        area_total = jnp.zeros(ice.shape, jnp.float32)
        for cat in range(CATS):
            area = area_ref[cat, at, :]
            load = load + area * fresh_ref[STACKED + cat, at, :]
            area_total = area_total + area
        load = ice * load
        forcing_ref[0, at, :] = drive_ref[0, at, :] + drive_ref[2, at, :]
        forcing_ref[1, at, :] = drive_ref[1, at, :] + drive_ref[3, at, :]
        forcing_ref[2, at, :] = cells_ref[at, :].astype(jnp.float32)
        forcing_ref[3, at, :] = load * jnp.exp(-20.0 * (1.0 - area_total))
        forcing_ref[4, at, :] = 0.9 * load

    def extra(team):
        def one(level, carry):
            tiles = tiles_of(team)
            picks = []
            for at in tiles:
                rank = lane + level * LANES - base_ref[at, :]
                inside = jnp.logical_and(rank >= 0, rank < count_ref[at, :])
                spot = jnp.take_along_axis(inverse_ref[at, :], jnp.where(inside, rank, 0), axis=1)
                picks.append((at, jnp.where(inside, spot, -1)))
            gather_team(picks, kept_ref, snow_ref, single_ref, gathered_a)
            solve_team(gathered_a, result_a)
            spread_team(tiles, level, place_ref, fresh_ref, result_a, fresh_ref)
            return carry

        return one

    sent = []
    for turn in range(TURNS):
        for copy in fetched[turn]:
            copy.wait()
        teams = [turn * PAIR + k for k in range(PAIR)]
        for k, team in enumerate(teams):
            gather_team([(at, spot_ref[at, :]) for at in tiles_of(team)], kept_ref, snow_ref, single_ref, buffers[k % 2][0])
        for k, team in enumerate(teams):
            solve_team(*buffers[k % 2])
        for k, team in enumerate(teams):
            spread_team(tiles_of(team), 0, place_ref, kept_ref, buffers[k % 2][1], fresh_ref)

        force(slice(turn * HEIGHT, turn * HEIGHT + HEIGHT))
        for copy in send(turn):
            copy.start()
            sent.append(copy)

    @pl.when(most > LANES)
    def _():
        for copy in sent:
            copy.wait()

        def again(team, carry):
            return lax.fori_loop(1, TEAM, extra(team), carry)

        lax.fori_loop(0, TILES // TEAM, again, 0)
        for turn in range(TURNS):
            force(slice(turn * HEIGHT, turn * HEIGHT + HEIGHT))
        for copy in sent:
            copy.start()

    def pack(tile, carry):
        group = lax.shift_right_logical(lane, 3)
        for out_ref, half, push in ((left_out, 0, 0), (right_out, 1, 8)):
            at = pl.ds(pl.multiple_of(tile * 8 + half * ROWS, 8), 8)
            packed = jnp.zeros((8, LANES), jnp.float32)
            for i in range(FIELDS):
                x = moving_ref[i, at, :] if i < 5 else forcing_ref[i - 5, at, :]
                turn = (8 * i + push) % LANES
                if turn:
                    x = pltpu.roll(x, turn, axis=1)
                packed = jnp.where(group == i, x, packed)
            out_ref[pl.ds(pl.multiple_of(tile * 8, 8), 8), :] = packed
        return carry

    lax.fori_loop(0, ROWS // 8, pack, 0, unroll=True)
    for copy in sent:
        copy.wait()


def halo_tile(west, east, field, rows):
    lane = lax.broadcasted_iota(jnp.int32, (rows, LANES), 1)
    east_side = pltpu.roll(east, (LANES - 8 * field) % LANES, axis=1) if field else east
    west_side = pltpu.roll(west, (120 - 8 * field) % LANES, axis=1)
    zero = jnp.zeros((rows, LANES), jnp.float32)
    return jnp.where(lane < DEEP, east_side, jnp.where(lane >= LANES - DEEP, west_side, zero))


def rows_kernel(
    spot_ref, vel_low, stress_low, forcing_low, west_low, east_low,
    vel_high, stress_high, forcing_high, west_high, east_high, even_out, odd_out,
):
    even = lax.rem(spot_ref[0], 2) == 0

    def fill(to_low, to_high):
        for out, vel_ref, stress_ref, forcing_ref, west_ref, east_ref in (
            (to_low, vel_low, stress_low, forcing_low, west_low, east_low),
            (to_high, vel_high, stress_high, forcing_high, west_high, east_high),
        ):
            for i in range(FIELDS):
                ref, at = (vel_ref, i) if i < 2 else (stress_ref, i - 2) if i < 5 else (forcing_ref, i - 5)
                out[i, 0] = ref[at, :, :LANES]
                out[i, 1] = ref[at, :, LANES:]
                out[i, 2] = halo_tile(west_ref[...], east_ref[...], i, DEEP)

    @pl.when(even)
    def _():
        fill(odd_out, even_out)

    @pl.when(jnp.logical_not(even))
    def _():
        fill(even_out, odd_out)


def flip(x):
    lane = (LANES - 1) - lax.broadcasted_iota(jnp.int32, (DEEP, LANES), 1)
    turned = jnp.take_along_axis(x, lane, axis=1)
    return jnp.concatenate([turned[i : i + 1] for i in range(DEEP - 1, -1, -1)], axis=0)


def motion_kernel(
    spot_ref, vel_hbm, stress_hbm, forcing_hbm, west_ref, east_ref, even_ref, odd_ref,
    vel_out, stress_out, state_ref, in_sem, out_sem,
):
    spot = spot_ref[0]
    even = lax.rem(spot, 2) == 0
    top = spot == spot_ref[1] - 1
    low = slice(DEEP, 2 * DEEP)
    mid = slice(2 * DEEP, 2 * DEEP + ROWS)
    high = slice(2 * DEEP + ROWS, 3 * DEEP + ROWS)
    copies = []
    for tile in range(2):
        span = slice(tile * LANES, tile * LANES + LANES)
        for number, (source, target) in enumerate((
            (vel_hbm, state_ref.at[0:2, tile, mid, :]),
            (stress_hbm, state_ref.at[2:5, tile, mid, :]),
            (forcing_hbm, state_ref.at[5:10, tile, mid, :]),
        )):
            copy = pltpu.make_async_copy(source.at[:, :, span], target, in_sem.at[tile, number])
            copy.start()
            copies.append(copy)
    blank = jnp.zeros((DEEP, LANES), jnp.float32)
    for i in range(FIELDS):
        for tile in range(3):
            state_ref[i, tile, :DEEP, :] = blank
            state_ref[i, tile, TALL - DEEP :, :] = blank
        state_ref[i, 2, mid, :] = halo_tile(west_ref[...], east_ref[...], i, ROWS)

    @pl.when(even)
    def _():
        for i in range(FIELDS):
            for tile in range(3):
                state_ref[i, tile, high, :] = even_ref[i, tile]
                state_ref[i, tile, low, :] = odd_ref[i, tile]

    @pl.when(jnp.logical_not(even))
    def _():
        for i in range(FIELDS):
            for tile in range(3):
                state_ref[i, tile, low, :] = even_ref[i, tile]
                state_ref[i, tile, high, :] = odd_ref[i, tile]

    @pl.when(top)
    def _():
        for i in range(FIELDS):
            for tile, source in ((0, 1), (1, 0), (2, 2)):
                turned = flip(odd_ref[i, source])
                state_ref[i, tile, high, :] = -turned if i in (0, 1, 5, 6) else turned

    for copy in copies:
        copy.wait()
    bands = (TALL - 2 * DEEP) // BAND
    lane = lax.broadcasted_iota(jnp.int32, (BAND, LANES), 1)
    is_first = lane == 0
    is_final = lane == LANES - 1

    def prepare(band, carry):
        start = pl.multiple_of(DEEP + band * BAND, 8)
        at = pl.ds(start, BAND)
        row = lax.broadcasted_iota(jnp.int32, (BAND, LANES), 0) + (start - 2 * DEEP) + spot * ROWS
        whole = spot_ref[1] * ROWS
        row = jnp.where(row >= whole, 2 * whole - 1 - row, row)
        latitude = row.astype(jnp.float32) + 0.5
        turn = 1.4 * jnp.sin(0.5 * jnp.pi * (2.0 * latitude / whole.astype(jnp.float32) - 1.0))
        for tile in range(3):
            mass = state_ref[9, tile, at, :]
            diagonal = mass + 1.0
            turning = turn * mass
            scale = state_ref[7, tile, at, :] / (diagonal * diagonal + turning * turning)
            state_ref[7, tile, at, :] = diagonal * scale
            state_ref[10, tile, at, :] = turning * scale
        return carry

    lax.fori_loop(0, bands, prepare, 0)

    def shift_x(parts):
        ahead = [pltpu.roll(x, LANES - 1, axis=1) for x in parts]
        behind = [pltpu.roll(x, 1, axis=1) for x in parts]
        return [
            jnp.where(is_final, ahead[(k + 1) % 3], ahead[k]) - jnp.where(is_first, behind[(k + 2) % 3], behind[k])
            for k in range(3)
        ]

    def shift_y(field, tile, start):
        return state_ref[field, tile, pl.ds(start + 1, BAND), :] - state_ref[field, tile, pl.ds(start - 1, BAND), :]

    def stresses(band, carry):
        start = pl.multiple_of(DEEP + band * BAND, 8)
        at = pl.ds(start, BAND)
        east_dx = shift_x([state_ref[0, k, at, :] for k in range(3)])
        north_dx = shift_x([state_ref[1, k, at, :] for k in range(3)])
        for k in range(3):
            north_dy = shift_y(1, k, start)
            diverge = 0.5 * (east_dx[k] + north_dy)
            tension = 0.5 * (east_dx[k] - north_dy)
            shearing = 0.5 * (shift_y(0, k, start) + north_dx[k])
            deform = diverge * diverge + 0.25 * (tension * tension + shearing * shearing) + 1.0
            strength = state_ref[8, k, at, :] * (1.0 / 3.0)
            bulk = strength * lax.rsqrt(deform)
            viscous = bulk * 0.25
            state_ref[2, k, at, :] = state_ref[2, k, at, :] * (2.0 / 3.0) + (bulk * diverge - strength)
            state_ref[3, k, at, :] = state_ref[3, k, at, :] * (2.0 / 3.0) + viscous * tension
            state_ref[4, k, at, :] = state_ref[4, k, at, :] * (2.0 / 3.0) + viscous * (0.5 * shearing)
        return carry

    def momentum(band, carry):
        start = pl.multiple_of(DEEP + band * BAND, 8)
        at = pl.ds(start, BAND)
        up = pl.ds(start + 1, BAND)
        down = pl.ds(start - 1, BAND)
        normal_dx = shift_x([state_ref[2, k, at, :] + state_ref[3, k, at, :] for k in range(3)])
        shear_dx = shift_x([state_ref[4, k, at, :] for k in range(3)])
        for k in range(3):
            shear_dy = shift_y(4, k, start)
            normal_dy = (state_ref[2, k, up, :] - state_ref[3, k, up, :]) - (
                state_ref[2, k, down, :] - state_ref[3, k, down, :]
            )
            mass = state_ref[9, k, at, :]
            right_east = mass * state_ref[0, k, at, :] + (0.25 * normal_dx[k] + 0.5 * shear_dy) + state_ref[5, k, at, :]
            right_north = mass * state_ref[1, k, at, :] + (0.5 * shear_dx[k] + 0.25 * normal_dy) + state_ref[6, k, at, :]
            straight = state_ref[7, k, at, :]
            turned = state_ref[10, k, at, :]
            state_ref[0, k, at, :] = straight * right_east + turned * right_north
            state_ref[1, k, at, :] = straight * right_north - turned * right_east
        return carry

    def subcycle(turn, carry):
        lax.fori_loop(0, bands, stresses, 0)
        lax.fori_loop(0, bands, momentum, 0)
        return carry

    lax.fori_loop(0, SUB, subcycle, 0)
    sent = []
    for tile in range(2):
        span = slice(tile * LANES, tile * LANES + LANES)
        for number, (source, target) in enumerate((
            (state_ref.at[0:2, tile, mid, :], vel_out),
            (state_ref.at[2:5, tile, mid, :], stress_out),
        )):
            copy = pltpu.make_async_copy(source, target.at[:, :, span], out_sem.at[tile, number])
            copy.start()
            sent.append(copy)
    for copy in sent:
        copy.wait()


def per_device(
    layer_temps, ice_thick, snow_thick, ice_area, air_temp, ocean_heat,
    velocity, stress, wind_stress, ocean_current, ocean_mask, ice_cols,
):
    f32 = jnp.float32
    i32 = jnp.int32
    smem = pl.BlockSpec(memory_space=pltpu.SMEM)
    vmem = pl.BlockSpec(memory_space=pltpu.VMEM)
    here = pl.BlockSpec(memory_space=pl.ANY)
    listed = ice_cols.reshape(1, -1)

    def flat(n, kind=f32):
        return pltpu.VMEM((n, FLAT, LANES), kind)

    one = pltpu.VMEM((FLAT, LANES), i32)
    temps_new, thick_new, forcing, left, right = pl.pallas_call(
        thermo_kernel,
        name="thermo",
        in_specs=[vmem] + [here] * 11,
        out_specs=[here, here, here, vmem, vmem],
        out_shape=[
            jax.ShapeDtypeStruct((STACKED, ROWS, COLS), f32),
            jax.ShapeDtypeStruct((CATS, ROWS, COLS), f32),
            jax.ShapeDtypeStruct((5, ROWS, COLS), f32),
            jax.ShapeDtypeStruct((ROWS, LANES), f32),
            jax.ShapeDtypeStruct((ROWS, LANES), f32),
        ],
        scratch_shapes=[
            flat(KEPT), flat(KEPT), flat(CATS), flat(CATS), flat(2), flat(5), flat(4), one, flat(5),
            pltpu.VMEM((FLAT, LANES), f32), one, one, one, one, one,
            pltpu.VMEM((KEPT + CATS + 2, 8, LANES), f32),
            pltpu.VMEM((KEPT + CATS + 2, 8, LANES), f32),
            pltpu.VMEM((KEPT, 8, LANES), f32),
            pltpu.VMEM((KEPT, 8, LANES), f32),
            pltpu.SemaphoreType.DMA((TURNS, 11)),
            pltpu.SemaphoreType.DMA((TURNS, 3)),
        ],
    )(
        listed, layer_temps, ice_thick, snow_thick, ice_area, air_temp, ocean_heat,
        velocity, stress, wind_stress, ocean_current, ocean_mask,
    )
    n_bx = lax.axis_size("bx")
    n_by = lax.axis_size("by")
    west = lax.ppermute(right, "bx", [(q, (q + 1) % n_bx) for q in range(n_bx)])
    east = lax.ppermute(left, "bx", [((q + 1) % n_bx, q) for q in range(n_bx)])

    spot = jnp.stack([lax.axis_index("by"), jnp.int32(n_by)]).astype(i32)
    band = jax.ShapeDtypeStruct((FIELDS, 3, DEEP, LANES), f32)

    def slab(n, block):
        return pl.BlockSpec((n, DEEP, COLS), lambda i: (0, block, 0))

    def edge(block):
        return pl.BlockSpec((DEEP, LANES), lambda i: (block, 0))

    final = ROWS // DEEP - 1
    halo = pl.BlockSpec((FIELDS, 3, DEEP, LANES), lambda i: (0, 0, 0, 0))
    even_rows, odd_rows = pl.pallas_call(
        rows_kernel,
        name="edge_rows",
        grid=(1,),
        in_specs=[smem]
        + [slab(2, 0), slab(3, 0), slab(5, 0), edge(0), edge(0)]
        + [slab(2, final), slab(3, final), slab(5, final), edge(final), edge(final)],
        out_specs=[halo, halo],
        out_shape=[band, band],
    )(spot, velocity, stress, forcing, west, east, velocity, stress, forcing, west, east)

    def at(p, q):
        return q * n_by + p

    even_pairs, odd_pairs = [], []
    for q in range(n_bx):
        for p in range(0, n_by, 2):
            even_pairs += [(at(p, q), at(p + 1, q)), (at(p + 1, q), at(p, q))]
        for p in range(1, n_by - 1, 2):
            odd_pairs += [(at(p, q), at(p + 1, q)), (at(p + 1, q), at(p, q))]
        odd_pairs.append((at(n_by - 1, q), at(n_by - 1, n_bx - 1 - q)))
    even_halo = lax.ppermute(even_rows, ("bx", "by"), even_pairs)
    odd_halo = lax.ppermute(odd_rows, ("bx", "by"), odd_pairs)

    velocity_new, stress_new = pl.pallas_call(
        motion_kernel,
        name="motion",
        in_specs=[smem] + [here] * 3 + [vmem] * 4,
        out_specs=[here, here],
        out_shape=[
            jax.ShapeDtypeStruct((2, ROWS, COLS), f32),
            jax.ShapeDtypeStruct((3, ROWS, COLS), f32),
        ],
        scratch_shapes=[
            pltpu.VMEM((FIELDS + 1, 3, TALL, LANES), f32),
            pltpu.SemaphoreType.DMA((2, 3)),
            pltpu.SemaphoreType.DMA((2, 2)),
        ],
    )(spot, velocity, stress, forcing, west, east, even_halo, odd_halo)
    return temps_new, thick_new, velocity_new, stress_new


def solution(mesh):
    grid3 = P(None, "by", "bx")
    grid2 = P("by", "bx")
    in_specs = (
        grid3, grid3, grid3, grid3, grid2, grid2, grid3, grid3, grid3, grid3, grid2,
        P("by", "bx", None),
    )
    return jax.shard_map(
        per_device, mesh=mesh, in_specs=in_specs, out_specs=(grid3,) * 4, check_vma=False
    )
```

```python
import functools

import jax
import jax.numpy as jnp
from jax import lax
from jax.experimental import pallas as pl
from jax.experimental.pallas import tpu as pltpu
from jax.sharding import PartitionSpec as P

ITERS = 4
SUB = 4
CATS = 5
LAYERS = 8
ROWS = 128
COLS = 256
DEEP = 8
FIELDS = 11
TALL = ROWS + 4 * DEEP
BAND = 144
LANES = 128
TILES = 32
FLAT = TILES * 8
STACKED = CATS * LAYERS
KEPT = STACKED + CATS
TEAM = 4
PAIR = 2
TURNS = TILES // (TEAM * PAIR)
HEIGHT = FLAT // TURNS
BLOCK = 13

FREEZING = -1.8
K_BASE = 2.03
K_GAIN = 0.47
K_SNOW = 0.31
ROOT = K_BASE / K_GAIN


def inverse(x):
    return 1.0 / x


def column(temps, thick, snow, air):
    depth = thick * (1.0 / (LAYERS - 1))
    square = depth * depth
    slope = square * (360.0 / K_GAIN)
    floor = square * (10.5 / K_GAIN)
    inv_depth = inverse(depth)
    snow_res = snow * inv_depth * (K_GAIN / K_SNOW)
    top_link = depth * (0.5 / K_GAIN) * inverse(snow * (0.5 / K_SNOW) + 0.05)
    snow_cap = snow * depth * (10.5 / K_GAIN)
    top_sum = snow_cap + top_link
    top_right = snow_cap * temps[0] + top_link * air
    current = list(temps)
    last = LAYERS - 1
    for repeat in range(ITERS):
        soft = [None] + [inverse(current[i] * current[i] + 1.0) for i in range(1, LAYERS)]
        conduct = [None] + [soft[i] + ROOT for i in range(1, LAYERS)]
        res = [snow_res] + [inverse(conduct[i]) for i in range(1, LAYERS)]
        cap = [None] + [slope * soft[i] + floor for i in range(1, LAYERS)]
        link = [res[i] + res[i + 1] for i in range(last)]
        ratio = [None] * LAYERS
        value = [None] * LAYERS
        down, down_flux = None, None
        for i in range(0, 4):
            total = top_sum if i == 0 else cap[i] + down
            right = top_right if i == 0 else cap[i] * temps[i] + down_flux
            ratio[i] = inverse(total * link[i] + 1.0)
            down = total * ratio[i]
            down_flux = right * ratio[i]
            value[i] = link[i] * down_flux
        up = conduct[last]
        up_flux = up * FREEZING
        for i in range(last, 4, -1):
            total = cap[i] + up
            right = cap[i] * temps[i] + up_flux
            ratio[i] = inverse(total * link[i - 1] + 1.0)
            up = total * ratio[i]
            up_flux = right * ratio[i]
            value[i] = link[i - 1] * up_flux
        renewed = [None] * LAYERS
        renewed[4] = (cap[4] * temps[4] + (down_flux + up_flux)) * inverse(cap[4] + (down + up))
        for i in range(3, -1, -1):
            if i > 0 or repeat == ITERS - 1:
                renewed[i] = value[i] + ratio[i] * renewed[i + 1]
        for i in range(5, LAYERS):
            renewed[i] = value[i] + ratio[i] * renewed[i - 1]
        current = renewed
    base = inverse(current[last] * current[last] + 1.0) + ROOT
    growth = (2.0 * K_GAIN * 0.0005) * (base * inv_depth) * (FREEZING - current[last])
    return current, growth


def draw_mask(list_ref):
    step = 512
    total = jnp.zeros((FLAT, LANES), jnp.float32)
    row_iota = lax.broadcasted_iota(jnp.int32, (FLAT, step), 0).astype(jnp.float32).astype(jnp.bfloat16)
    lane_iota = lax.broadcasted_iota(jnp.int32, (LANES, step), 0).astype(jnp.float32).astype(jnp.bfloat16)
    one = jnp.bfloat16(1.0)
    zero = jnp.bfloat16(0.0)
    for start in range(0, list_ref.shape[1], step):
        cells = list_ref[:, start : start + step]
        row = lax.shift_right_arithmetic(cells, 8) + (lax.bitwise_and(cells, 128))
        row = jnp.where(cells >= 0, row, -1).astype(jnp.float32).astype(jnp.bfloat16)
        lane = lax.bitwise_and(cells, 127).astype(jnp.float32).astype(jnp.bfloat16)
        total = total + lax.dot_general(
            jnp.where(row_iota == row, one, zero),
            jnp.where(lane_iota == lane, one, zero),
            (((1,), (1,)), ((), ())),
            preferred_element_type=jnp.float32,
        )
    return total


def index_cells(list_ref, mask_ref, base_ref, count_ref, inverse_ref, place_ref, spot_ref):
    mask = draw_mask(list_ref)
    mask_ref[...] = mask
    small = mask.astype(jnp.bfloat16)
    before = lax.broadcasted_iota(jnp.int32, (LANES, LANES), 0) < lax.broadcasted_iota(jnp.int32, (LANES, LANES), 1)
    before = before.astype(jnp.float32).astype(jnp.bfloat16)
    prefix = jnp.dot(small, before, preferred_element_type=jnp.float32).astype(jnp.int32)
    count = jnp.dot(small, jnp.ones((LANES, LANES), jnp.bfloat16), preferred_element_type=jnp.float32).astype(jnp.int32)
    count_ref[...] = count
    most = jnp.zeros((8, LANES), jnp.int32)
    running = most
    for t in range(TILES):
        if t % TEAM == 0:
            running = jnp.zeros((8, LANES), jnp.int32)
        base_ref[8 * t : 8 * t + 8, :] = running
        running = running + count[8 * t : 8 * t + 8]
        most = jnp.maximum(most, running)
    wide_lane = lax.broadcasted_iota(jnp.int32, (FLAT, LANES), 1)
    moved = jnp.where(mask > 0.5, (wide_lane - prefix) * 256 + wide_lane, 0)
    for bit in range(7):
        probe = 256 << bit
        near = pltpu.roll(moved, LANES - (1 << bit), axis=1)
        moved = jnp.where(
            lax.bitwise_and(near, probe) != 0,
            near,
            jnp.where(lax.bitwise_and(moved, probe) != 0, 0, moved),
        )
    inverse = lax.bitwise_and(moved, LANES - 1)
    inverse_ref[...] = inverse
    base = base_ref[...]
    place_ref[...] = jnp.where(mask > 0.5, prefix + base, -1)
    lane = lax.broadcasted_iota(jnp.int32, (8, LANES), 1)
    for t in range(TILES):
        here = slice(8 * t, 8 * t + 8)
        rank = lane - base_ref[here, :]
        inside = jnp.logical_and(rank >= 0, rank < count[here])
        spot = jnp.take_along_axis(inverse[here], jnp.where(inside, rank, 0), axis=1)
        spot_ref[here, :] = jnp.where(inside, spot, -1)
    return jnp.max(most)


def gather_team(picks, kept_ref, snow_ref, single_ref, gathered_ref):
    planes = [(kept_ref, p) for p in range(KEPT)]
    planes += [(snow_ref, p) for p in range(CATS)] + [(single_ref, 0), (single_ref, 1)]
    for start in range(0, len(planes), BLOCK):
        block = planes[start : start + BLOCK]
        values = [None] * len(block)
        for at, spot in picks:
            inside = spot >= 0
            spot = jnp.maximum(spot, 0)
            for k, (ref, p) in enumerate(block):
                value = jnp.take_along_axis(ref[p, at, :], spot, axis=1)
                values[k] = value if values[k] is None else jnp.where(inside, value, values[k])
        for k, value in enumerate(values):
            gathered_ref[start + k] = value


def solve_team(gathered_ref, result_ref):
    air = gathered_ref[KEPT + CATS]
    heat = gathered_ref[KEPT + CATS + 1]
    for cat in range(CATS):
        temps = [gathered_ref[cat * LAYERS + i] for i in range(LAYERS)]
        thick = gathered_ref[STACKED + cat]
        current, growth = column(temps, thick, gathered_ref[KEPT + cat], air)
        for i in range(LAYERS):
            result_ref[cat * LAYERS + i] = current[i]
        result_ref[STACKED + cat] = thick + (growth - 0.0005 * heat)


def field_of(i, moving, forcing):
    return (moving, i) if i < 5 else (forcing, i - 5)


def spread_team(tiles, level, place_ref, source_ref, result_ref, fresh_ref, planes, skip=0):
    for at in tiles:
        place = place_ref[at, :] - level * LANES
        inside = jnp.logical_and(place >= 0, place < LANES)
        spot = jnp.where(inside, place, 0)
        for p in planes:
            value = jnp.take_along_axis(result_ref[p], spot, axis=1)
            fresh_ref[p - skip, at, :] = jnp.where(inside, value, source_ref[p, at, :])


def thermo_kernel(
    list_ref, temps_hbm, thick_hbm, snow_hbm, area_hbm, air_hbm, heat_hbm,
    vel_hbm, stress_hbm, wind_hbm, ocean_hbm, cells_hbm,
    thick_out, forcing_out, result_out, place_out, left_out, right_out,
    kept_ref, fresh_ref, snow_ref, area_ref, single_ref, moving_ref, drive_ref, cells_ref, forcing_ref,
    mask_ref, base_ref, count_ref, inverse_ref, place_ref, spot_ref,
    gathered_a, gathered_b, result_ref, in_sem, out_sem, result_sem, extra_sem,
):
    band = lax.axis_index("by")
    north = lax.axis_size("by") * ROWS

    def fetch(turn):
        half, inner = turn // (TURNS // 2), turn % (TURNS // 2)
        span = slice(half * LANES, half * LANES + LANES)
        there = slice(inner * HEIGHT, inner * HEIGHT + HEIGHT)
        rows = slice(turn * HEIGHT, turn * HEIGHT + HEIGHT)
        copies = []
        for source, target in (
            (temps_hbm, kept_ref.at[:STACKED]),
            (thick_hbm, kept_ref.at[STACKED:]),
            (snow_hbm, snow_ref),
            (air_hbm, single_ref.at[0]),
            (heat_hbm, single_ref.at[1]),
            (area_hbm, area_ref),
            (wind_hbm, drive_ref.at[0:2]),
            (ocean_hbm, drive_ref.at[2:4]),
            (cells_hbm, cells_ref),
            (vel_hbm, moving_ref.at[0:2]),
            (stress_hbm, moving_ref.at[2:5]),
        ):
            sem = in_sem.at[turn, len(copies)]
            if len(source.shape) == 3:
                copies.append(pltpu.make_async_copy(source.at[:, there, span], target.at[:, rows, :], sem))
            else:
                copies.append(pltpu.make_async_copy(source.at[there, span], target.at[rows, :], sem))
        return copies

    def send(turn):
        half, inner = turn // (TURNS // 2), turn % (TURNS // 2)
        span = slice(half * LANES, half * LANES + LANES)
        there = slice(inner * HEIGHT, inner * HEIGHT + HEIGHT)
        rows = slice(turn * HEIGHT, turn * HEIGHT + HEIGHT)
        return [
            pltpu.make_async_copy(fresh_ref.at[:, rows, :], thick_out.at[:, there, span], out_sem.at[turn, 0]),
            pltpu.make_async_copy(forcing_ref.at[:, rows, :], forcing_out.at[:, there, span], out_sem.at[turn, 1]),
        ]

    fetched = [fetch(turn) for turn in range(TURNS)]
    for copies in fetched:
        for copy in copies:
            copy.start()
    most = index_cells(list_ref, mask_ref, base_ref, count_ref, inverse_ref, place_ref, spot_ref)
    sent = [pltpu.make_async_copy(place_ref, place_out, result_sem.at[TILES // TEAM])]
    sent[0].start()
    lane = lax.broadcasted_iota(jnp.int32, (8, LANES), 1)
    buffers = (gathered_a, gathered_b)
    thick_planes = range(STACKED, KEPT)

    def tiles_of(team):
        return [pl.ds(pl.multiple_of((team * TEAM + u) * 8, 8), 8) for u in range(TEAM)]

    def force(turn):
        at = slice(turn * HEIGHT, turn * HEIGHT + HEIGHT)
        ice = mask_ref[at, :]
        load = jnp.zeros(ice.shape, jnp.float32)
        area_total = jnp.zeros(ice.shape, jnp.float32)
        for cat in range(CATS):
            area = area_ref[cat, at, :]
            load = load + area * fresh_ref[cat, at, :]
            area_total = area_total + area
        load = ice * load
        mass = 0.9 * load
        row = lax.broadcasted_iota(jnp.int32, (HEIGHT, LANES), 0) + (turn % (TURNS // 2)) * HEIGHT + band * ROWS
        latitude = row.astype(jnp.float32) + 0.5
        turning = 1.4 * jnp.sin(0.5 * jnp.pi * (2.0 * latitude / north - 1.0)) * mass
        diagonal = mass + 1.0
        scale = cells_ref[at, :].astype(jnp.float32) / (diagonal * diagonal + turning * turning)
        forcing_ref[0, at, :] = drive_ref[0, at, :] + drive_ref[2, at, :]
        forcing_ref[1, at, :] = drive_ref[1, at, :] + drive_ref[3, at, :]
        forcing_ref[2, at, :] = diagonal * scale
        forcing_ref[3, at, :] = load * jnp.exp(-20.0 * (1.0 - area_total))
        forcing_ref[4, at, :] = mass
        forcing_ref[5, at, :] = turning * scale

    def extra(team):
        def one(level, carry):
            tiles = tiles_of(team)
            picks = []
            for at in tiles:
                rank = lane + level * LANES - base_ref[at, :]
                inside = jnp.logical_and(rank >= 0, rank < count_ref[at, :])
                spot = jnp.take_along_axis(inverse_ref[at, :], jnp.where(inside, rank, 0), axis=1)
                picks.append((at, jnp.where(inside, spot, -1)))
            gather_team(picks, kept_ref, snow_ref, single_ref, gathered_a)
            solve_team(gathered_a, result_ref.at[TILES // TEAM])
            for at in tiles:
                place = place_ref[at, :] - level * LANES
                inside = jnp.logical_and(place >= 0, place < LANES)
                spot = jnp.where(inside, place, 0)
                for p in thick_planes:
                    value = jnp.take_along_axis(result_ref[TILES // TEAM, p], spot, axis=1)
                    fresh_ref[p - STACKED, at, :] = jnp.where(inside, value, fresh_ref[p - STACKED, at, :])
            copy = pltpu.make_async_copy(result_ref.at[TILES // TEAM, :STACKED], result_out.at[level, team], extra_sem)
            copy.start()
            copy.wait()
            return carry

        return one

    for turn in range(TURNS):
        for copy in fetched[turn]:
            copy.wait()
        teams = [turn * PAIR + k for k in range(PAIR)]
        for k, team in enumerate(teams):
            gather_team([(at, spot_ref[at, :]) for at in tiles_of(team)], kept_ref, snow_ref, single_ref, buffers[k % 2])
        for k, team in enumerate(teams):
            solve_team(buffers[k % 2], result_ref.at[team])
        for k, team in enumerate(teams):
            spread_team(tiles_of(team), 0, place_ref, kept_ref, result_ref.at[team], fresh_ref, thick_planes, STACKED)
            copy = pltpu.make_async_copy(result_ref.at[team, :STACKED], result_out.at[0, team], result_sem.at[team])
            copy.start()
            sent.append(copy)
        force(turn)
        for copy in send(turn):
            copy.start()
            sent.append(copy)

    @pl.when(most > LANES)
    def _():
        for copy in sent:
            copy.wait()

        def again(team, carry):
            return lax.fori_loop(1, TEAM, extra(team), carry)

        lax.fori_loop(0, TILES // TEAM, again, 0)
        for turn in range(TURNS):
            force(turn)
        for copy in sent:
            copy.start()

    def pack(tile, carry):
        group = lax.shift_right_logical(lane, 3)
        for out_ref, half, push in ((left_out, 0, 0), (right_out, 1, 8)):
            at = pl.ds(pl.multiple_of(tile * 8 + half * ROWS, 8), 8)
            packed = jnp.zeros((8, LANES), jnp.float32)
            for i in range(FIELDS):
                ref, k = field_of(i, moving_ref, forcing_ref)
                x = ref[k, at, :]
                turn = (8 * i + push) % LANES
                if turn:
                    x = pltpu.roll(x, turn, axis=1)
                packed = jnp.where(group == i, x, packed)
            out_ref[pl.ds(pl.multiple_of(tile * 8, 8), 8), :] = packed
        return carry

    lax.fori_loop(0, ROWS // 8, pack, 0, unroll=True)
    for copy in sent:
        copy.wait()


def temps_kernel(half, temps_hbm, result_hbm, place_hbm, *rest):
    temps_out, kept_ref, fresh_ref, place_ref, result_ref, in_sem, out_sem, extra_sem = rest[-8:]
    teams = TILES // TEAM // 2
    height = TEAM * 8
    span = slice(half * LANES, half * LANES + LANES)
    rows = slice(half * ROWS, half * ROWS + ROWS)
    whole = pltpu.make_async_copy(place_hbm.at[rows, :], place_ref, extra_sem)
    whole.start()
    fetched = []
    for k in range(teams):
        here = slice(k * height, k * height + height)
        fetched.append([
            pltpu.make_async_copy(temps_hbm.at[:, here, span], kept_ref.at[:, here, :], in_sem.at[k, 0]),
            pltpu.make_async_copy(result_hbm.at[0, half * teams + k], result_ref.at[k], in_sem.at[k, 1]),
        ])
    for copies in fetched:
        for copy in copies:
            copy.start()
    whole.wait()
    sent = []
    for k in range(teams):
        for copy in fetched[k]:
            copy.wait()
        here = slice(k * height, k * height + height)
        tiles = [slice(k * height + 8 * u, k * height + 8 * u + 8) for u in range(TEAM)]
        spread_team(tiles, 0, place_ref, kept_ref, result_ref.at[k], fresh_ref, range(STACKED))
        copy = pltpu.make_async_copy(fresh_ref.at[:, here, :], temps_out.at[:, here, span], out_sem.at[k])
        copy.start()
        sent.append(copy)

    @pl.when(jnp.max(place_ref[...]) >= LANES)
    def _():
        for copy in sent:
            copy.wait()

        def again(step, carry):
            team = lax.div(step, TEAM - 1)
            level = lax.rem(step, TEAM - 1) + 1
            copy = pltpu.make_async_copy(result_hbm.at[level, half * teams + team], result_ref.at[0], extra_sem)
            copy.start()
            copy.wait()
            for u in range(TEAM):
                at = pl.ds(pl.multiple_of(team * height + 8 * u, 8), 8)
                place = place_ref[at, :] - level * LANES
                inside = jnp.logical_and(place >= 0, place < LANES)
                spot = jnp.where(inside, place, 0)
                for p in range(STACKED):
                    value = jnp.take_along_axis(result_ref[0, p], spot, axis=1)
                    fresh_ref[p, at, :] = jnp.where(inside, value, fresh_ref[p, at, :])
            return carry

        lax.fori_loop(0, teams * (TEAM - 1), again, 0)
        for copy in sent:
            copy.start()

    for copy in sent:
        copy.wait()


def halo_tile(west, east, field, rows):
    lane = lax.broadcasted_iota(jnp.int32, (rows, LANES), 1)
    east_side = pltpu.roll(east, (LANES - 8 * field) % LANES, axis=1) if field else east
    west_side = pltpu.roll(west, (120 - 8 * field) % LANES, axis=1)
    zero = jnp.zeros((rows, LANES), jnp.float32)
    return jnp.where(lane < DEEP, east_side, jnp.where(lane >= LANES - DEEP, west_side, zero))


def rows_kernel(
    vel_low, stress_low, forcing_low, west_low, east_low,
    vel_high, stress_high, forcing_high, west_high, east_high, even_out, odd_out,
):
    even = lax.rem(lax.axis_index("by"), 2) == 0

    def fill(to_low, to_high):
        for out, vel_ref, stress_ref, forcing_ref, west_ref, east_ref in (
            (to_low, vel_low, stress_low, forcing_low, west_low, east_low),
            (to_high, vel_high, stress_high, forcing_high, west_high, east_high),
        ):
            for i in range(FIELDS):
                ref, at = (vel_ref, i) if i < 2 else (stress_ref, i - 2) if i < 5 else (forcing_ref, i - 5)
                out[i, 0] = ref[at, :, :LANES]
                out[i, 1] = ref[at, :, LANES:]
                out[i, 2] = halo_tile(west_ref[...], east_ref[...], i, DEEP)

    @pl.when(even)
    def _():
        fill(odd_out, even_out)

    @pl.when(jnp.logical_not(even))
    def _():
        fill(even_out, odd_out)


def flip(x):
    lane = (LANES - 1) - lax.broadcasted_iota(jnp.int32, (DEEP, LANES), 1)
    turned = jnp.take_along_axis(x, lane, axis=1)
    return jnp.concatenate([turned[i : i + 1] for i in range(DEEP - 1, -1, -1)], axis=0)


def motion_kernel(
    vel_hbm, stress_hbm, forcing_hbm, west_hbm, east_hbm, even_hbm, odd_hbm,
    vel_out, stress_out, state_ref, west_ref, east_ref, even_ref, odd_ref, in_sem, halo_sem, out_sem,
):
    spot = lax.axis_index("by")
    even = lax.rem(spot, 2) == 0
    top = spot == lax.axis_size("by") - 1
    halos = []
    for source, target in ((west_hbm, west_ref), (east_hbm, east_ref), (even_hbm, even_ref), (odd_hbm, odd_ref)):
        copy = pltpu.make_async_copy(source, target, halo_sem.at[len(halos)])
        copy.start()
        halos.append(copy)
    low = slice(DEEP, 2 * DEEP)
    mid = slice(2 * DEEP, 2 * DEEP + ROWS)
    high = slice(2 * DEEP + ROWS, 3 * DEEP + ROWS)
    copies = []
    for tile in range(2):
        span = slice(tile * LANES, tile * LANES + LANES)
        for number, (source, target) in enumerate((
            (vel_hbm, state_ref.at[0:2, tile, mid, :]),
            (stress_hbm, state_ref.at[2:5, tile, mid, :]),
            (forcing_hbm, state_ref.at[5:11, tile, mid, :]),
        )):
            copy = pltpu.make_async_copy(source.at[:, :, span], target, in_sem.at[tile, number])
            copy.start()
            copies.append(copy)
    for copy in halos:
        copy.wait()
    blank = jnp.zeros((DEEP, LANES), jnp.float32)
    for i in range(FIELDS):
        for tile in range(3):
            state_ref[i, tile, :DEEP, :] = blank
            state_ref[i, tile, TALL - DEEP :, :] = blank
        state_ref[i, 2, mid, :] = halo_tile(west_ref[...], east_ref[...], i, ROWS)

    @pl.when(even)
    def _():
        for i in range(FIELDS):
            for tile in range(3):
                state_ref[i, tile, high, :] = even_ref[i, tile]
                state_ref[i, tile, low, :] = odd_ref[i, tile]

    @pl.when(jnp.logical_not(even))
    def _():
        for i in range(FIELDS):
            for tile in range(3):
                state_ref[i, tile, low, :] = even_ref[i, tile]
                state_ref[i, tile, high, :] = odd_ref[i, tile]

    @pl.when(top)
    def _():
        for i in range(FIELDS):
            for tile, source in ((0, 1), (1, 0), (2, 2)):
                turned = flip(odd_ref[i, source])
                state_ref[i, tile, high, :] = -turned if i in (0, 1, 5, 6) else turned

    for copy in copies:
        copy.wait()
    bands = (TALL - 2 * DEEP) // BAND
    lane = lax.broadcasted_iota(jnp.int32, (BAND, LANES), 1)
    is_first = lane == 0
    is_final = lane == LANES - 1

    def shift_x(parts):
        ahead = [pltpu.roll(x, LANES - 1, axis=1) for x in parts]
        behind = [pltpu.roll(x, 1, axis=1) for x in parts]
        return [
            jnp.where(is_final, ahead[(k + 1) % 3], ahead[k]) - jnp.where(is_first, behind[(k + 2) % 3], behind[k])
            for k in range(3)
        ]

    def shift_y(field, tile, start):
        return state_ref[field, tile, pl.ds(start + 1, BAND), :] - state_ref[field, tile, pl.ds(start - 1, BAND), :]

    def stresses(band, carry):
        start = pl.multiple_of(DEEP + band * BAND, 8)
        at = pl.ds(start, BAND)
        east_dx = shift_x([state_ref[0, k, at, :] for k in range(3)])
        north_dx = shift_x([state_ref[1, k, at, :] for k in range(3)])
        for k in range(3):
            north_dy = shift_y(1, k, start)
            diverge = 0.5 * (east_dx[k] + north_dy)
            tension = 0.5 * (east_dx[k] - north_dy)
            shearing = 0.5 * (shift_y(0, k, start) + north_dx[k])
            deform = diverge * diverge + 0.25 * (tension * tension + shearing * shearing) + 1.0
            strength = state_ref[8, k, at, :] * (1.0 / 3.0)
            bulk = strength * lax.rsqrt(deform)
            viscous = bulk * 0.25
            state_ref[2, k, at, :] = state_ref[2, k, at, :] * (2.0 / 3.0) + (bulk * diverge - strength)
            state_ref[3, k, at, :] = state_ref[3, k, at, :] * (2.0 / 3.0) + viscous * tension
            state_ref[4, k, at, :] = state_ref[4, k, at, :] * (2.0 / 3.0) + viscous * (0.5 * shearing)
        return carry

    def momentum(band, carry):
        start = pl.multiple_of(DEEP + band * BAND, 8)
        at = pl.ds(start, BAND)
        up = pl.ds(start + 1, BAND)
        down = pl.ds(start - 1, BAND)
        normal_dx = shift_x([state_ref[2, k, at, :] + state_ref[3, k, at, :] for k in range(3)])
        shear_dx = shift_x([state_ref[4, k, at, :] for k in range(3)])
        for k in range(3):
            shear_dy = shift_y(4, k, start)
            normal_dy = (state_ref[2, k, up, :] - state_ref[3, k, up, :]) - (
                state_ref[2, k, down, :] - state_ref[3, k, down, :]
            )
            mass = state_ref[9, k, at, :]
            right_east = mass * state_ref[0, k, at, :] + (0.25 * normal_dx[k] + 0.5 * shear_dy) + state_ref[5, k, at, :]
            right_north = mass * state_ref[1, k, at, :] + (0.5 * shear_dx[k] + 0.25 * normal_dy) + state_ref[6, k, at, :]
            straight = state_ref[7, k, at, :]
            turned = state_ref[10, k, at, :]
            state_ref[0, k, at, :] = straight * right_east + turned * right_north
            state_ref[1, k, at, :] = straight * right_north - turned * right_east
        return carry

    def subcycle(turn, carry):
        lax.fori_loop(0, bands, stresses, 0)
        lax.fori_loop(0, bands, momentum, 0)
        return carry

    lax.fori_loop(0, SUB - 1, subcycle, 0)
    lax.fori_loop(0, bands, stresses, 0)
    sent = []

    def send(number, fields, target):
        for tile in range(2):
            span = slice(tile * LANES, tile * LANES + LANES)
            copy = pltpu.make_async_copy(
                state_ref.at[fields, tile, mid, :], target.at[:, :, span], out_sem.at[tile, number]
            )
            copy.start()
            sent.append(copy)

    send(0, slice(2, 5), stress_out)
    lax.fori_loop(0, bands, momentum, 0)
    send(1, slice(0, 2), vel_out)
    for copy in sent:
        copy.wait()


def per_device(
    layer_temps, ice_thick, snow_thick, ice_area, air_temp, ocean_heat,
    velocity, stress, wind_stress, ocean_current, ocean_mask, ice_cols,
):
    f32 = jnp.float32
    i32 = jnp.int32
    vmem = pl.BlockSpec(memory_space=pltpu.VMEM)
    here = pl.BlockSpec(memory_space=pl.ANY)
    listed = ice_cols.reshape(1, -1)

    def flat(n, kind=f32):
        return pltpu.VMEM((n, FLAT, LANES), kind)

    one = pltpu.VMEM((FLAT, LANES), i32)
    teams = TILES // TEAM
    thick_new, forcing, result, place, left, right = pl.pallas_call(
        thermo_kernel,
        name="thermo",
        in_specs=[vmem] + [here] * 11,
        out_specs=[here, here, here, here, vmem, vmem],
        out_shape=[
            jax.ShapeDtypeStruct((CATS, ROWS, COLS), f32),
            jax.ShapeDtypeStruct((6, ROWS, COLS), f32),
            jax.ShapeDtypeStruct((TEAM, teams, STACKED, 8, LANES), f32),
            jax.ShapeDtypeStruct((FLAT, LANES), i32),
            jax.ShapeDtypeStruct((ROWS, LANES), f32),
            jax.ShapeDtypeStruct((ROWS, LANES), f32),
        ],
        scratch_shapes=[
            flat(KEPT), flat(CATS), flat(CATS), flat(CATS), flat(2), flat(5), flat(4), one, flat(6),
            pltpu.VMEM((FLAT, LANES), f32), one, one, one, one, one,
            pltpu.VMEM((KEPT + CATS + 2, 8, LANES), f32),
            pltpu.VMEM((KEPT + CATS + 2, 8, LANES), f32),
            pltpu.VMEM((teams + 1, KEPT, 8, LANES), f32),
            pltpu.SemaphoreType.DMA((TURNS, 11)),
            pltpu.SemaphoreType.DMA((TURNS, 2)),
            pltpu.SemaphoreType.DMA((teams + 1,)),
            pltpu.SemaphoreType.DMA,
        ],
    )(
        listed, layer_temps, ice_thick, snow_thick, ice_area, air_temp, ocean_heat,
        velocity, stress, wind_stress, ocean_current, ocean_mask,
    )

    def renew(half, *before):
        return pl.pallas_call(
            functools.partial(temps_kernel, half),
            name="temps_west" if half == 0 else "temps_east",
            in_specs=[here] * (3 + len(before)),
            out_specs=here,
            out_shape=jax.ShapeDtypeStruct((STACKED, ROWS, COLS), f32),
            input_output_aliases={3: 0} if before else {},
            cost_estimate=pl.CostEstimate(flops=20_000_000, transcendentals=0, bytes_accessed=6_000_000),
            scratch_shapes=[
                pltpu.VMEM((STACKED, ROWS, LANES), f32),
                pltpu.VMEM((STACKED, ROWS, LANES), f32),
                pltpu.VMEM((ROWS, LANES), i32),
                pltpu.VMEM((teams // 2, STACKED, 8, LANES), f32),
                pltpu.SemaphoreType.DMA((teams // 2, 2)),
                pltpu.SemaphoreType.DMA((teams // 2,)),
                pltpu.SemaphoreType.DMA,
            ],
        )(layer_temps, result, place, *before)

    n_bx = lax.axis_size("bx")
    n_by = lax.axis_size("by")
    west = lax.ppermute(right, "bx", [(q, (q + 1) % n_bx) for q in range(n_bx)])
    east = lax.ppermute(left, "bx", [((q + 1) % n_bx, q) for q in range(n_bx)])
    temps_part = renew(0)
    band = jax.ShapeDtypeStruct((FIELDS, 3, DEEP, LANES), f32)

    def slab(n, block):
        return pl.BlockSpec((n, DEEP, COLS), lambda i: (0, block, 0))

    def edge(block):
        return pl.BlockSpec((DEEP, LANES), lambda i: (block, 0))

    final = ROWS // DEEP - 1
    halo = pl.BlockSpec((FIELDS, 3, DEEP, LANES), lambda i: (0, 0, 0, 0))
    even_rows, odd_rows = pl.pallas_call(
        rows_kernel,
        name="edge_rows",
        grid=(1,),
        in_specs=[slab(2, 0), slab(3, 0), slab(6, 0), edge(0), edge(0)]
        + [slab(2, final), slab(3, final), slab(6, final), edge(final), edge(final)],
        out_specs=[halo, halo],
        out_shape=[band, band],
    )(velocity, stress, forcing, west, east, velocity, stress, forcing, west, east)

    def at(p, q):
        return q * n_by + p

    even_pairs, odd_pairs = [], []
    for q in range(n_bx):
        for p in range(0, n_by, 2):
            even_pairs += [(at(p, q), at(p + 1, q)), (at(p + 1, q), at(p, q))]
        for p in range(1, n_by - 1, 2):
            odd_pairs += [(at(p, q), at(p + 1, q)), (at(p + 1, q), at(p, q))]
        odd_pairs.append((at(n_by - 1, q), at(n_by - 1, n_bx - 1 - q)))
    even_rows, odd_rows, temps_part = lax.optimization_barrier((even_rows, odd_rows, temps_part))
    odd_halo = lax.ppermute(odd_rows, ("bx", "by"), odd_pairs)
    even_halo = lax.ppermute(even_rows, ("bx", "by"), even_pairs)
    temps_new = renew(1, temps_part)
    edge_shape = pltpu.VMEM((ROWS, LANES), f32)
    band_shape = pltpu.VMEM((FIELDS, 3, DEEP, LANES), f32)
    velocity_new, stress_new = pl.pallas_call(
        motion_kernel,
        name="motion",
        in_specs=[here] * 7,
        out_specs=[here, here],
        out_shape=[
            jax.ShapeDtypeStruct((2, ROWS, COLS), f32),
            jax.ShapeDtypeStruct((3, ROWS, COLS), f32),
        ],
        scratch_shapes=[
            pltpu.VMEM((FIELDS, 3, TALL, LANES), f32),
            edge_shape, edge_shape, band_shape, band_shape,
            pltpu.SemaphoreType.DMA((2, 3)),
            pltpu.SemaphoreType.DMA((4,)),
            pltpu.SemaphoreType.DMA((2, 2)),
        ],
    )(velocity, stress, forcing, west, east, even_halo, odd_halo)
    return temps_new, thick_new, velocity_new, stress_new


def solution(mesh):
    grid3 = P(None, "by", "bx")
    grid2 = P("by", "bx")
    in_specs = (
        grid3, grid3, grid3, grid3, grid2, grid2, grid3, grid3, grid3, grid3, grid2,
        P("by", "bx", None),
    )
    return jax.shard_map(
        per_device, mesh=mesh, in_specs=in_specs, out_specs=(grid3,) * 4, check_vma=False
    )
```

```python
import functools

import jax
import jax.numpy as jnp
from jax import lax
from jax.experimental import pallas as pl
from jax.experimental.pallas import tpu as pltpu
from jax.sharding import PartitionSpec as P

ITERS = 4
SUB = 4
CATS = 5
LAYERS = 8
ROWS = 128
COLS = 256
DEEP = 8
FIELDS = 11
TALL = ROWS + 4 * DEEP
BAND = 144
LANES = 128
TILES = 32
FLAT = TILES * 8
STACKED = CATS * LAYERS
KEPT = STACKED + CATS
TEAM = 4
PAIR = 2
TURNS = TILES // (TEAM * PAIR)
HEIGHT = ROWS // TURNS
BLOCK = 13

FREEZING = -1.8
K_BASE = 2.03
K_GAIN = 0.47
K_SNOW = 0.31
ROOT = K_BASE / K_GAIN


def inverse(x):
    return 1.0 / x


def column(temps, thick, snow, air):
    depth = thick * (1.0 / (LAYERS - 1))
    square = depth * depth
    slope = square * (360.0 / K_GAIN)
    floor = square * (10.5 / K_GAIN)
    inv_depth = inverse(depth)
    snow_res = snow * inv_depth * (K_GAIN / K_SNOW)
    top_link = depth * (0.5 / K_GAIN) * inverse(snow * (0.5 / K_SNOW) + 0.05)
    snow_cap = snow * depth * (10.5 / K_GAIN)
    top_sum = snow_cap + top_link
    top_right = snow_cap * temps[0] + top_link * air
    current = list(temps)
    last = LAYERS - 1
    for repeat in range(ITERS):
        soft = [None] + [inverse(current[i] * current[i] + 1.0) for i in range(1, LAYERS)]
        conduct = [None] + [soft[i] + ROOT for i in range(1, LAYERS)]
        res = [snow_res] + [inverse(conduct[i]) for i in range(1, LAYERS)]
        cap = [None] + [slope * soft[i] + floor for i in range(1, LAYERS)]
        link = [res[i] + res[i + 1] for i in range(last)]
        ratio = [None] * LAYERS
        value = [None] * LAYERS
        down, down_flux = None, None
        for i in range(0, 4):
            total = top_sum if i == 0 else cap[i] + down
            right = top_right if i == 0 else cap[i] * temps[i] + down_flux
            ratio[i] = inverse(total * link[i] + 1.0)
            down = total * ratio[i]
            down_flux = right * ratio[i]
            value[i] = link[i] * down_flux
        up = conduct[last]
        up_flux = up * FREEZING
        for i in range(last, 4, -1):
            total = cap[i] + up
            right = cap[i] * temps[i] + up_flux
            ratio[i] = inverse(total * link[i - 1] + 1.0)
            up = total * ratio[i]
            up_flux = right * ratio[i]
            value[i] = link[i - 1] * up_flux
        renewed = [None] * LAYERS
        renewed[4] = (cap[4] * temps[4] + (down_flux + up_flux)) * inverse(cap[4] + (down + up))
        for i in range(3, -1, -1):
            if i > 0 or repeat == ITERS - 1:
                renewed[i] = value[i] + ratio[i] * renewed[i + 1]
        for i in range(5, LAYERS):
            renewed[i] = value[i] + ratio[i] * renewed[i - 1]
        current = renewed
    base = inverse(current[last] * current[last] + 1.0) + ROOT
    growth = (2.0 * K_GAIN * 0.0005) * (base * inv_depth) * (FREEZING - current[last])
    return current, growth


def draw_mask(list_ref):
    step = 512
    total = jnp.zeros((FLAT, LANES), jnp.float32)
    row_iota = lax.broadcasted_iota(jnp.int32, (FLAT, step), 0).astype(jnp.float32).astype(jnp.bfloat16)
    lane_iota = lax.broadcasted_iota(jnp.int32, (LANES, step), 0).astype(jnp.float32).astype(jnp.bfloat16)
    one = jnp.bfloat16(1.0)
    zero = jnp.bfloat16(0.0)
    for start in range(0, list_ref.shape[1], step):
        cells = list_ref[:, start : start + step]
        row = (
            lax.bitwise_and(lax.shift_right_arithmetic(cells, 7), 0xF0)
            + lax.bitwise_and(lax.shift_right_arithmetic(cells, 4), 8)
            + lax.bitwise_and(lax.shift_right_arithmetic(cells, 8), 7)
        )
        row = jnp.where(cells >= 0, row, -1).astype(jnp.float32).astype(jnp.bfloat16)
        lane = lax.bitwise_and(cells, 127).astype(jnp.float32).astype(jnp.bfloat16)
        total = total + lax.dot_general(
            jnp.where(row_iota == row, one, zero),
            jnp.where(lane_iota == lane, one, zero),
            (((1,), (1,)), ((), ())),
            preferred_element_type=jnp.float32,
        )
    return total


def index_cells(list_ref, mask_ref, base_ref, count_ref, inverse_ref, place_ref, spot_ref):
    mask = draw_mask(list_ref)
    mask_ref[...] = mask
    small = mask.astype(jnp.bfloat16)
    before = lax.broadcasted_iota(jnp.int32, (LANES, LANES), 0) < lax.broadcasted_iota(jnp.int32, (LANES, LANES), 1)
    before = before.astype(jnp.float32).astype(jnp.bfloat16)
    prefix = jnp.dot(small, before, preferred_element_type=jnp.float32).astype(jnp.int32)
    count = jnp.dot(small, jnp.ones((LANES, LANES), jnp.bfloat16), preferred_element_type=jnp.float32).astype(jnp.int32)
    count_ref[...] = count
    most = jnp.zeros((8, LANES), jnp.int32)
    running = most
    for t in range(TILES):
        if t % TEAM == 0:
            running = jnp.zeros((8, LANES), jnp.int32)
        base_ref[8 * t : 8 * t + 8, :] = running
        running = running + count[8 * t : 8 * t + 8]
        most = jnp.maximum(most, running)
    wide_lane = lax.broadcasted_iota(jnp.int32, (FLAT, LANES), 1)
    moved = jnp.where(mask > 0.5, (wide_lane - prefix) * 256 + wide_lane, 0)
    for bit in range(7):
        probe = 256 << bit
        near = pltpu.roll(moved, LANES - (1 << bit), axis=1)
        moved = jnp.where(
            lax.bitwise_and(near, probe) != 0,
            near,
            jnp.where(lax.bitwise_and(moved, probe) != 0, 0, moved),
        )
    inverse = lax.bitwise_and(moved, LANES - 1)
    inverse_ref[...] = inverse
    base = base_ref[...]
    place_ref[...] = jnp.where(mask > 0.5, prefix + base, -1)
    lane = lax.broadcasted_iota(jnp.int32, (8, LANES), 1)
    for t in range(TILES):
        here = slice(8 * t, 8 * t + 8)
        rank = lane - base_ref[here, :]
        inside = jnp.logical_and(rank >= 0, rank < count[here])
        spot = jnp.take_along_axis(inverse[here], jnp.where(inside, rank, 0), axis=1)
        spot_ref[here, :] = jnp.where(inside, spot, -1)
    return jnp.max(most)


def gather_team(picks, kept_ref, snow_ref, single_ref, gathered_ref):
    planes = [(kept_ref, p) for p in range(KEPT)]
    planes += [(snow_ref, p) for p in range(CATS)] + [(single_ref, 0), (single_ref, 1)]
    for start in range(0, len(planes), BLOCK):
        block = planes[start : start + BLOCK]
        values = [None] * len(block)
        for (rows, lanes), spot in picks:
            inside = spot >= 0
            spot = jnp.maximum(spot, 0)
            for k, (ref, p) in enumerate(block):
                value = jnp.take_along_axis(ref[p, rows, lanes], spot, axis=1)
                values[k] = value if values[k] is None else jnp.where(inside, value, values[k])
        for k, value in enumerate(values):
            gathered_ref[start + k] = value


def solve_team(gathered_ref, result_ref):
    air = gathered_ref[KEPT + CATS]
    heat = gathered_ref[KEPT + CATS + 1]
    for cat in range(CATS):
        temps = [gathered_ref[cat * LAYERS + i] for i in range(LAYERS)]
        thick = gathered_ref[STACKED + cat]
        current, growth = column(temps, thick, gathered_ref[KEPT + cat], air)
        for i in range(LAYERS):
            result_ref[cat * LAYERS + i] = current[i]
        result_ref[STACKED + cat] = thick + (growth - 0.0005 * heat)


def tiles_of(team):
    tiles = []
    for u in range(TEAM):
        row = (team * (TEAM // 2) + u // 2) * 8
        flat = (team * TEAM + u) * 8
        if not isinstance(team, int):
            row, flat = pl.multiple_of(row, 8), pl.multiple_of(flat, 8)
        lanes = slice((u % 2) * LANES, (u % 2) * LANES + LANES)
        tiles.append(((pl.ds(row, 8), lanes), pl.ds(flat, 8)))
    return tiles


def spread_team(tiles, level, place_ref, source_ref, result_ref, fresh_ref, planes, skip=0):
    for (rows, lanes), flat in tiles:
        place = place_ref[flat, :] - level * LANES
        inside = jnp.logical_and(place >= 0, place < LANES)
        spot = jnp.where(inside, place, 0)
        for p in planes:
            value = jnp.take_along_axis(result_ref[p], spot, axis=1)
            before = source_ref[p, rows, lanes] if source_ref is not None else fresh_ref[p - skip, rows, lanes]
            fresh_ref[p - skip, rows, lanes] = jnp.where(inside, value, before)


def thermo_kernel(
    list_hbm, temps_hbm, thick_hbm, snow_hbm, area_hbm, air_hbm, heat_hbm,
    vel_hbm, stress_hbm, wind_hbm, ocean_hbm, cells_hbm,
    thick_out, state_out, result_out, place_out, left_out, right_out,
    list_ref, kept_ref, fresh_ref, snow_ref, area_ref, single_ref, drive_ref, cells_ref, state_ref,
    mask_ref, base_ref, count_ref, inverse_ref, place_ref, spot_ref,
    gathered_a, gathered_b, result_ref, edge_ref, in_sem, out_sem, move_sem, result_sem, extra_sem,
):
    band = lax.axis_index("by")
    north = lax.axis_size("by") * ROWS
    teams = TILES // TEAM
    listing = pltpu.make_async_copy(list_hbm, list_ref, extra_sem)
    listing.start()

    def fetch(turn):
        rows = slice(turn * HEIGHT, turn * HEIGHT + HEIGHT)
        copies = []
        for source, target in (
            (temps_hbm, kept_ref.at[:STACKED]),
            (thick_hbm, kept_ref.at[STACKED:]),
            (snow_hbm, snow_ref),
            (air_hbm, single_ref.at[0]),
            (heat_hbm, single_ref.at[1]),
            (area_hbm, area_ref),
            (wind_hbm, drive_ref.at[0:2]),
            (ocean_hbm, drive_ref.at[2:4]),
            (cells_hbm, cells_ref),
        ):
            sem = in_sem.at[turn, len(copies)]
            if len(source.shape) == 3:
                copies.append(pltpu.make_async_copy(source.at[:, rows, :], target.at[:, rows, :], sem))
            else:
                copies.append(pltpu.make_async_copy(source.at[rows, :], target.at[rows, :], sem))
        return copies

    def send(turn):
        rows = slice(turn * HEIGHT, turn * HEIGHT + HEIGHT)
        return [
            pltpu.make_async_copy(fresh_ref.at[:, rows, :], thick_out.at[:, rows, :], out_sem.at[turn, 0]),
            pltpu.make_async_copy(state_ref.at[:, :, rows, :], state_out.at[:, :, rows, :], out_sem.at[turn, 1]),
        ]

    fetched = [fetch(turn) for turn in range(TURNS)]
    moved = []
    for half in range(2):
        span = slice(half * LANES, half * LANES + LANES)
        moved.append(pltpu.make_async_copy(vel_hbm.at[:, :, span], state_ref.at[0:2, half], move_sem.at[half, 0]))
        moved.append(pltpu.make_async_copy(stress_hbm.at[:, :, span], state_ref.at[2:5, half], move_sem.at[half, 1]))
    for copies in fetched + [moved]:
        for copy in copies:
            copy.start()
    listing.wait()
    most = index_cells(list_ref, mask_ref, base_ref, count_ref, inverse_ref, place_ref, spot_ref)
    sent = [pltpu.make_async_copy(place_ref, place_out, result_sem.at[teams])]
    sent[0].start()
    lane = lax.broadcasted_iota(jnp.int32, (8, LANES), 1)
    buffers = (gathered_a, gathered_b)
    thick_planes = range(STACKED, KEPT)

    def force(turn):
        for inner in range(HEIGHT // 8):
            start = turn * HEIGHT + inner * 8
            rows = slice(start, start + 8)
            row = lax.broadcasted_iota(jnp.int32, (8, LANES), 0) + start + band * ROWS
            latitude = row.astype(jnp.float32) + 0.5
            coriolis = 1.4 * jnp.sin(0.5 * jnp.pi * (2.0 * latitude / north - 1.0))
            for half in range(2):
                lanes = slice(half * LANES, half * LANES + LANES)
                ice = mask_ref[2 * start + 8 * half : 2 * start + 8 * half + 8, :]
                load = jnp.zeros(ice.shape, jnp.float32)
                area_total = jnp.zeros(ice.shape, jnp.float32)
                for cat in range(CATS):
                    area = area_ref[cat, rows, lanes]
                    load = load + area * fresh_ref[cat, rows, lanes]
                    area_total = area_total + area
                load = ice * load
                mass = 0.9 * load
                turning = coriolis * mass
                diagonal = mass + 1.0
                scale = cells_ref[rows, lanes].astype(jnp.float32) / (diagonal * diagonal + turning * turning)
                state_ref[5, half, rows, :] = drive_ref[0, rows, lanes] + drive_ref[2, rows, lanes]
                state_ref[6, half, rows, :] = drive_ref[1, rows, lanes] + drive_ref[3, rows, lanes]
                state_ref[7, half, rows, :] = diagonal * scale
                state_ref[8, half, rows, :] = load * jnp.exp(-20.0 * (1.0 - area_total))
                state_ref[9, half, rows, :] = mass
                state_ref[10, half, rows, :] = turning * scale

    def extra(team):
        def one(level, carry):
            tiles = tiles_of(team)
            picks = []
            for at, flat in tiles:
                rank = lane + level * LANES - base_ref[flat, :]
                inside = jnp.logical_and(rank >= 0, rank < count_ref[flat, :])
                spot = jnp.take_along_axis(inverse_ref[flat, :], jnp.where(inside, rank, 0), axis=1)
                picks.append((at, jnp.where(inside, spot, -1)))
            gather_team(picks, kept_ref, snow_ref, single_ref, gathered_a)
            solve_team(gathered_a, result_ref.at[teams])
            spread_team(tiles, level, place_ref, None, result_ref.at[teams], fresh_ref, thick_planes, STACKED)
            copy = pltpu.make_async_copy(result_ref.at[teams, :STACKED], result_out.at[level, team], extra_sem)
            copy.start()
            copy.wait()
            return carry

        return one

    for turn in range(TURNS):
        for copy in fetched[turn]:
            copy.wait()
        if turn == 0:
            for copy in moved:
                copy.wait()
        mine = [turn * PAIR + k for k in range(PAIR)]
        for k, team in enumerate(mine):
            picks = [(at, spot_ref[flat, :]) for at, flat in tiles_of(team)]
            gather_team(picks, kept_ref, snow_ref, single_ref, buffers[k % 2])
        for k, team in enumerate(mine):
            solve_team(buffers[k % 2], result_ref.at[team])
        for k, team in enumerate(mine):
            spread_team(tiles_of(team), 0, place_ref, kept_ref, result_ref.at[team], fresh_ref, thick_planes, STACKED)
            copy = pltpu.make_async_copy(result_ref.at[team, :STACKED], result_out.at[0, team], result_sem.at[team])
            copy.start()
            sent.append(copy)
        force(turn)
        for copy in send(turn):
            copy.start()
            sent.append(copy)

    @pl.when(most > LANES)
    def _():
        for copy in sent:
            copy.wait()

        def again(team, carry):
            return lax.fori_loop(1, TEAM, extra(team), carry)

        lax.fori_loop(0, teams, again, 0)
        for turn in range(TURNS):
            force(turn)
        for copy in sent:
            copy.start()

    group = lax.shift_right_logical(lane, 3)
    edges = []
    for half, push, target in ((1, 8, right_out), (0, 0, left_out)):
        for tile in range(ROWS // 8):
            packed = jnp.zeros((8, LANES), jnp.float32)
            for i in range(FIELDS):
                x = state_ref[i, half, 8 * tile : 8 * tile + 8, :]
                turn = (8 * i + push) % LANES
                if turn:
                    x = pltpu.roll(x, turn, axis=1)
                packed = jnp.where(group == i, x, packed)
            edge_ref[half, 8 * tile : 8 * tile + 8, :] = packed
        copy = pltpu.make_async_copy(edge_ref.at[half], target, move_sem.at[half, 2])
        copy.start()
        edges.append(copy)
    for copy in sent + edges:
        copy.wait()


def temps_kernel(half, temps_hbm, result_hbm, place_hbm, *rest):
    temps_out, kept_ref, fresh_ref, place_ref, result_ref, in_sem, out_sem, extra_sem = rest[-8:]
    teams = TILES // TEAM // 2
    height = TEAM * 4
    skip = half * (ROWS // 2)
    whole = pltpu.make_async_copy(place_hbm.at[half * ROWS : half * ROWS + ROWS, :], place_ref, extra_sem)
    whole.start()
    fetched = []
    for k in range(teams):
        here = slice(k * height, k * height + height)
        there = slice(skip + k * height, skip + k * height + height)
        fetched.append([
            pltpu.make_async_copy(temps_hbm.at[:, there, :], kept_ref.at[:, here, :], in_sem.at[k, 0]),
            pltpu.make_async_copy(result_hbm.at[0, half * teams + k], result_ref.at[k], in_sem.at[k, 1]),
        ])
    for copies in fetched:
        for copy in copies:
            copy.start()
    whole.wait()
    sent = []
    for k in range(teams):
        for copy in fetched[k]:
            copy.wait()
        here = slice(k * height, k * height + height)
        there = slice(skip + k * height, skip + k * height + height)
        spread_team(tiles_of(k), 0, place_ref, kept_ref, result_ref.at[k], fresh_ref, range(STACKED))
        copy = pltpu.make_async_copy(fresh_ref.at[:, here, :], temps_out.at[:, there, :], out_sem.at[k])
        copy.start()
        sent.append(copy)

    @pl.when(jnp.max(place_ref[...]) >= LANES)
    def _():
        for copy in sent:
            copy.wait()

        def again(step, carry):
            team = lax.div(step, TEAM - 1)
            level = lax.rem(step, TEAM - 1) + 1
            copy = pltpu.make_async_copy(result_hbm.at[level, half * teams + team], result_ref.at[0], extra_sem)
            copy.start()
            copy.wait()
            spread_team(tiles_of(team), level, place_ref, None, result_ref.at[0], fresh_ref, range(STACKED))
            return carry

        lax.fori_loop(0, teams * (TEAM - 1), again, 0)
        for copy in sent:
            copy.start()

    for copy in sent:
        copy.wait()


def halo_tile(west, east, field, rows):
    lane = lax.broadcasted_iota(jnp.int32, (rows, LANES), 1)
    east_side = pltpu.roll(east, (LANES - 8 * field) % LANES, axis=1) if field else east
    west_side = pltpu.roll(west, (120 - 8 * field) % LANES, axis=1)
    zero = jnp.zeros((rows, LANES), jnp.float32)
    return jnp.where(lane < DEEP, east_side, jnp.where(lane >= LANES - DEEP, west_side, zero))


def rows_kernel(state_low, west_low, east_low, state_high, west_high, east_high, even_out, odd_out):
    even = lax.rem(lax.axis_index("by"), 2) == 0

    def fill(to_low, to_high):
        for out, state_ref, west_ref, east_ref in (
            (to_low, state_low, west_low, east_low),
            (to_high, state_high, west_high, east_high),
        ):
            for i in range(FIELDS):
                out[i, 0] = state_ref[i, 0]
                out[i, 1] = state_ref[i, 1]
                out[i, 2] = halo_tile(west_ref[...], east_ref[...], i, DEEP)

    @pl.when(even)
    def _():
        fill(odd_out, even_out)

    @pl.when(jnp.logical_not(even))
    def _():
        fill(even_out, odd_out)


def flip(x):
    lane = (LANES - 1) - lax.broadcasted_iota(jnp.int32, (DEEP, LANES), 1)
    turned = jnp.take_along_axis(x, lane, axis=1)
    return jnp.concatenate([turned[i : i + 1] for i in range(DEEP - 1, -1, -1)], axis=0)


def motion_kernel(
    state_hbm, west_hbm, east_hbm, even_hbm, odd_hbm,
    vel_out, stress_out, state_ref, west_ref, east_ref, even_ref, odd_ref, in_sem, halo_sem, out_sem,
):
    spot = lax.axis_index("by")
    even = lax.rem(spot, 2) == 0
    top = spot == lax.axis_size("by") - 1
    halos = []
    for source, target in ((west_hbm, west_ref), (east_hbm, east_ref), (even_hbm, even_ref), (odd_hbm, odd_ref)):
        copy = pltpu.make_async_copy(source, target, halo_sem.at[len(halos)])
        copy.start()
        halos.append(copy)
    low = slice(DEEP, 2 * DEEP)
    mid = slice(2 * DEEP, 2 * DEEP + ROWS)
    high = slice(2 * DEEP + ROWS, 3 * DEEP + ROWS)
    copies = []
    for tile in range(2):
        copy = pltpu.make_async_copy(state_hbm.at[:, tile], state_ref.at[:, tile, mid, :], in_sem.at[tile])
        copy.start()
        copies.append(copy)
    for copy in halos:
        copy.wait()
    blank = jnp.zeros((DEEP, LANES), jnp.float32)
    for i in range(FIELDS):
        for tile in range(3):
            state_ref[i, tile, :DEEP, :] = blank
            state_ref[i, tile, TALL - DEEP :, :] = blank
        state_ref[i, 2, mid, :] = halo_tile(west_ref[...], east_ref[...], i, ROWS)

    @pl.when(even)
    def _():
        for i in range(FIELDS):
            for tile in range(3):
                state_ref[i, tile, high, :] = even_ref[i, tile]
                state_ref[i, tile, low, :] = odd_ref[i, tile]

    @pl.when(jnp.logical_not(even))
    def _():
        for i in range(FIELDS):
            for tile in range(3):
                state_ref[i, tile, low, :] = even_ref[i, tile]
                state_ref[i, tile, high, :] = odd_ref[i, tile]

    @pl.when(top)
    def _():
        for i in range(FIELDS):
            for tile, source in ((0, 1), (1, 0), (2, 2)):
                turned = flip(odd_ref[i, source])
                state_ref[i, tile, high, :] = -turned if i in (0, 1, 5, 6) else turned

    for copy in copies:
        copy.wait()
    bands = (TALL - 2 * DEEP) // BAND
    lane = lax.broadcasted_iota(jnp.int32, (BAND, LANES), 1)
    is_first = lane == 0
    is_final = lane == LANES - 1

    def shift_x(parts):
        ahead = [pltpu.roll(x, LANES - 1, axis=1) for x in parts]
        behind = [pltpu.roll(x, 1, axis=1) for x in parts]
        return [
            jnp.where(is_final, ahead[(k + 1) % 3], ahead[k]) - jnp.where(is_first, behind[(k + 2) % 3], behind[k])
            for k in range(3)
        ]

    def shift_y(field, tile, start):
        return state_ref[field, tile, pl.ds(start + 1, BAND), :] - state_ref[field, tile, pl.ds(start - 1, BAND), :]

    def stresses(band, carry):
        start = pl.multiple_of(DEEP + band * BAND, 8)
        at = pl.ds(start, BAND)
        east_dx = shift_x([state_ref[0, k, at, :] for k in range(3)])
        north_dx = shift_x([state_ref[1, k, at, :] for k in range(3)])
        for k in range(3):
            north_dy = shift_y(1, k, start)
            diverge = 0.5 * (east_dx[k] + north_dy)
            tension = 0.5 * (east_dx[k] - north_dy)
            shearing = 0.5 * (shift_y(0, k, start) + north_dx[k])
            deform = diverge * diverge + 0.25 * (tension * tension + shearing * shearing) + 1.0
            strength = state_ref[8, k, at, :] * (1.0 / 3.0)
            bulk = strength * lax.rsqrt(deform)
            viscous = bulk * 0.25
            state_ref[2, k, at, :] = state_ref[2, k, at, :] * (2.0 / 3.0) + (bulk * diverge - strength)
            state_ref[3, k, at, :] = state_ref[3, k, at, :] * (2.0 / 3.0) + viscous * tension
            state_ref[4, k, at, :] = state_ref[4, k, at, :] * (2.0 / 3.0) + viscous * (0.5 * shearing)
        return carry

    def momentum(band, carry):
        start = pl.multiple_of(DEEP + band * BAND, 8)
        at = pl.ds(start, BAND)
        up = pl.ds(start + 1, BAND)
        down = pl.ds(start - 1, BAND)
        normal_dx = shift_x([state_ref[2, k, at, :] + state_ref[3, k, at, :] for k in range(3)])
        shear_dx = shift_x([state_ref[4, k, at, :] for k in range(3)])
        for k in range(3):
            shear_dy = shift_y(4, k, start)
            normal_dy = (state_ref[2, k, up, :] - state_ref[3, k, up, :]) - (
                state_ref[2, k, down, :] - state_ref[3, k, down, :]
            )
            mass = state_ref[9, k, at, :]
            right_east = mass * state_ref[0, k, at, :] + (0.25 * normal_dx[k] + 0.5 * shear_dy) + state_ref[5, k, at, :]
            right_north = mass * state_ref[1, k, at, :] + (0.5 * shear_dx[k] + 0.25 * normal_dy) + state_ref[6, k, at, :]
            straight = state_ref[7, k, at, :]
            turned = state_ref[10, k, at, :]
            state_ref[0, k, at, :] = straight * right_east + turned * right_north
            state_ref[1, k, at, :] = straight * right_north - turned * right_east
        return carry

    def subcycle(turn, carry):
        lax.fori_loop(0, bands, stresses, 0)
        lax.fori_loop(0, bands, momentum, 0)
        return carry

    lax.fori_loop(0, SUB - 1, subcycle, 0)
    lax.fori_loop(0, bands, stresses, 0)
    sent = []

    def send(number, fields, target):
        for tile in range(2):
            span = slice(tile * LANES, tile * LANES + LANES)
            copy = pltpu.make_async_copy(
                state_ref.at[fields, tile, mid, :], target.at[:, :, span], out_sem.at[tile, number]
            )
            copy.start()
            sent.append(copy)

    send(0, slice(2, 5), stress_out)
    lax.fori_loop(0, bands, momentum, 0)
    send(1, slice(0, 2), vel_out)
    for copy in sent:
        copy.wait()


def per_device(
    layer_temps, ice_thick, snow_thick, ice_area, air_temp, ocean_heat,
    velocity, stress, wind_stress, ocean_current, ocean_mask, ice_cols,
):
    f32 = jnp.float32
    i32 = jnp.int32
    here = pl.BlockSpec(memory_space=pl.ANY)
    listed = ice_cols.reshape(1, -1)

    def planes(n):
        return pltpu.VMEM((n, ROWS, COLS), f32)

    one = pltpu.VMEM((FLAT, LANES), i32)
    teams = TILES // TEAM
    thick_new, state, result, place, left, right = pl.pallas_call(
        thermo_kernel,
        name="thermo",
        in_specs=[here] * 12,
        out_specs=[here] * 6,
        out_shape=[
            jax.ShapeDtypeStruct((CATS, ROWS, COLS), f32),
            jax.ShapeDtypeStruct((FIELDS, 2, ROWS, LANES), f32),
            jax.ShapeDtypeStruct((TEAM, teams, STACKED, 8, LANES), f32),
            jax.ShapeDtypeStruct((FLAT, LANES), i32),
            jax.ShapeDtypeStruct((ROWS, LANES), f32),
            jax.ShapeDtypeStruct((ROWS, LANES), f32),
        ],
        scratch_shapes=[
            pltpu.VMEM(listed.shape, i32),
            planes(KEPT), planes(CATS), planes(CATS), planes(CATS), planes(2), planes(4),
            pltpu.VMEM((ROWS, COLS), i32), pltpu.VMEM((FIELDS, 2, ROWS, LANES), f32),
            pltpu.VMEM((FLAT, LANES), f32), one, one, one, one, one,
            pltpu.VMEM((KEPT + CATS + 2, 8, LANES), f32),
            pltpu.VMEM((KEPT + CATS + 2, 8, LANES), f32),
            pltpu.VMEM((teams + 1, KEPT, 8, LANES), f32),
            pltpu.VMEM((2, ROWS, LANES), f32),
            pltpu.SemaphoreType.DMA((TURNS, 9)),
            pltpu.SemaphoreType.DMA((TURNS, 2)),
            pltpu.SemaphoreType.DMA((2, 3)),
            pltpu.SemaphoreType.DMA((teams + 1,)),
            pltpu.SemaphoreType.DMA,
        ],
    )(
        listed, layer_temps, ice_thick, snow_thick, ice_area, air_temp, ocean_heat,
        velocity, stress, wind_stress, ocean_current, ocean_mask,
    )

    def renew(half, *before):
        return pl.pallas_call(
            functools.partial(temps_kernel, half),
            name="temps_low" if half == 0 else "temps_high",
            in_specs=[here] * (3 + len(before)),
            out_specs=here,
            out_shape=jax.ShapeDtypeStruct((STACKED, ROWS, COLS), f32),
            input_output_aliases={3: 0} if before else {},
            cost_estimate=pl.CostEstimate(flops=20_000_000, transcendentals=0, bytes_accessed=6_000_000),
            scratch_shapes=[
                pltpu.VMEM((STACKED, ROWS // 2, COLS), f32),
                pltpu.VMEM((STACKED, ROWS // 2, COLS), f32),
                pltpu.VMEM((ROWS, LANES), i32),
                pltpu.VMEM((teams // 2, STACKED, 8, LANES), f32),
                pltpu.SemaphoreType.DMA((teams // 2, 2)),
                pltpu.SemaphoreType.DMA((teams // 2,)),
                pltpu.SemaphoreType.DMA,
            ],
        )(layer_temps, result, place, *before)

    n_bx = lax.axis_size("bx")
    n_by = lax.axis_size("by")
    west = lax.ppermute(right, "bx", [(q, (q + 1) % n_bx) for q in range(n_bx)])
    east = lax.ppermute(left, "bx", [((q + 1) % n_bx, q) for q in range(n_bx)])
    temps_part = renew(0)
    band = jax.ShapeDtypeStruct((FIELDS, 3, DEEP, LANES), f32)

    def slab(block):
        return pl.BlockSpec((FIELDS, 2, DEEP, LANES), lambda i: (0, 0, block, 0))

    def edge(block):
        return pl.BlockSpec((DEEP, LANES), lambda i: (block, 0))

    final = ROWS // DEEP - 1
    halo = pl.BlockSpec((FIELDS, 3, DEEP, LANES), lambda i: (0, 0, 0, 0))
    even_rows, odd_rows = pl.pallas_call(
        rows_kernel,
        name="edge_rows",
        grid=(1,),
        in_specs=[slab(0), edge(0), edge(0), slab(final), edge(final), edge(final)],
        out_specs=[halo, halo],
        out_shape=[band, band],
    )(state, west, east, state, west, east)

    def at(p, q):
        return q * n_by + p

    even_pairs, odd_pairs = [], []
    for q in range(n_bx):
        for p in range(0, n_by, 2):
            even_pairs += [(at(p, q), at(p + 1, q)), (at(p + 1, q), at(p, q))]
        for p in range(1, n_by - 1, 2):
            odd_pairs += [(at(p, q), at(p + 1, q)), (at(p + 1, q), at(p, q))]
        odd_pairs.append((at(n_by - 1, q), at(n_by - 1, n_bx - 1 - q)))
    even_rows, odd_rows, temps_part = lax.optimization_barrier((even_rows, odd_rows, temps_part))
    odd_halo = lax.ppermute(odd_rows, ("bx", "by"), odd_pairs)
    even_halo = lax.ppermute(even_rows, ("bx", "by"), even_pairs)
    temps_new = renew(1, temps_part)
    edge_shape = pltpu.VMEM((ROWS, LANES), f32)
    band_shape = pltpu.VMEM((FIELDS, 3, DEEP, LANES), f32)
    velocity_new, stress_new = pl.pallas_call(
        motion_kernel,
        name="motion",
        in_specs=[here] * 5,
        out_specs=[here, here],
        out_shape=[
            jax.ShapeDtypeStruct((2, ROWS, COLS), f32),
            jax.ShapeDtypeStruct((3, ROWS, COLS), f32),
        ],
        scratch_shapes=[
            pltpu.VMEM((FIELDS, 3, TALL, LANES), f32),
            edge_shape, edge_shape, band_shape, band_shape,
            pltpu.SemaphoreType.DMA((2,)),
            pltpu.SemaphoreType.DMA((4,)),
            pltpu.SemaphoreType.DMA((2, 2)),
        ],
    )(state, west, east, even_halo, odd_halo)
    return temps_new, thick_new, velocity_new, stress_new


def solution(mesh):
    grid3 = P(None, "by", "bx")
    grid2 = P("by", "bx")
    in_specs = (
        grid3, grid3, grid3, grid3, grid2, grid2, grid3, grid3, grid3, grid3, grid2,
        P("by", "bx", None),
    )
    return jax.shard_map(
        per_device, mesh=mesh, in_specs=in_specs, out_specs=(grid3,) * 4, check_vma=False
    )
```

```python
import functools

import jax
import jax.numpy as jnp
from jax import lax
from jax.experimental import pallas as pl
from jax.experimental.pallas import tpu as pltpu
from jax.sharding import PartitionSpec as P

ITERS = 4
SUB = 4
CATS = 5
LAYERS = 8
ROWS = 128
COLS = 256
DEEP = 8
FIELDS = 11
TALL = ROWS + 4 * DEEP
BAND = 144
LANES = 128
TILES = 32
FLAT = TILES * 8
STACKED = CATS * LAYERS
KEPT = STACKED + CATS
TEAM = 4
PAIR = 2
TURNS = TILES // (TEAM * PAIR)
HEIGHT = FLAT // TURNS
BLOCK = 13

FREEZING = -1.8
K_BASE = 2.03
K_GAIN = 0.47
K_SNOW = 0.31
ROOT = K_BASE / K_GAIN


def inverse(x):
    return 1.0 / x


def column(temps, thick, snow, air):
    depth = thick * (1.0 / (LAYERS - 1))
    square = depth * depth
    slope = square * (360.0 / K_GAIN)
    floor = square * (10.5 / K_GAIN)
    inv_depth = inverse(depth)
    snow_res = snow * inv_depth * (K_GAIN / K_SNOW)
    top_link = depth * (0.5 / K_GAIN) * inverse(snow * (0.5 / K_SNOW) + 0.05)
    snow_cap = snow * depth * (10.5 / K_GAIN)
    top_sum = snow_cap + top_link
    top_right = snow_cap * temps[0] + top_link * air
    current = list(temps)
    last = LAYERS - 1
    for repeat in range(ITERS):
        soft = [None] + [inverse(current[i] * current[i] + 1.0) for i in range(1, LAYERS)]
        conduct = [None] + [soft[i] + ROOT for i in range(1, LAYERS)]
        res = [snow_res] + [inverse(conduct[i]) for i in range(1, LAYERS)]
        cap = [None] + [slope * soft[i] + floor for i in range(1, LAYERS)]
        link = [res[i] + res[i + 1] for i in range(last)]
        ratio = [None] * LAYERS
        value = [None] * LAYERS
        down, down_flux = None, None
        for i in range(0, 4):
            total = top_sum if i == 0 else cap[i] + down
            right = top_right if i == 0 else cap[i] * temps[i] + down_flux
            ratio[i] = inverse(total * link[i] + 1.0)
            down = total * ratio[i]
            down_flux = right * ratio[i]
            value[i] = link[i] * down_flux
        up = conduct[last]
        up_flux = up * FREEZING
        for i in range(last, 4, -1):
            total = cap[i] + up
            right = cap[i] * temps[i] + up_flux
            ratio[i] = inverse(total * link[i - 1] + 1.0)
            up = total * ratio[i]
            up_flux = right * ratio[i]
            value[i] = link[i - 1] * up_flux
        renewed = [None] * LAYERS
        renewed[4] = (cap[4] * temps[4] + (down_flux + up_flux)) * inverse(cap[4] + (down + up))
        for i in range(3, -1, -1):
            if i > 0 or repeat == ITERS - 1:
                renewed[i] = value[i] + ratio[i] * renewed[i + 1]
        for i in range(5, LAYERS):
            renewed[i] = value[i] + ratio[i] * renewed[i - 1]
        current = renewed
    base = inverse(current[last] * current[last] + 1.0) + ROOT
    growth = (2.0 * K_GAIN * 0.0005) * (base * inv_depth) * (FREEZING - current[last])
    return current, growth


def draw_mask(list_ref):
    step = 512
    total = jnp.zeros((FLAT, LANES), jnp.float32)
    row_iota = lax.broadcasted_iota(jnp.int32, (FLAT, step), 0).astype(jnp.float32).astype(jnp.bfloat16)
    lane_iota = lax.broadcasted_iota(jnp.int32, (LANES, step), 0).astype(jnp.float32).astype(jnp.bfloat16)
    one = jnp.bfloat16(1.0)
    zero = jnp.bfloat16(0.0)
    for start in range(0, list_ref.shape[1], step):
        cells = list_ref[:, start : start + step]
        row = lax.shift_right_arithmetic(cells, 8) + (lax.bitwise_and(cells, 128))
        row = jnp.where(cells >= 0, row, -1).astype(jnp.float32).astype(jnp.bfloat16)
        lane = lax.bitwise_and(cells, 127).astype(jnp.float32).astype(jnp.bfloat16)
        total = total + lax.dot_general(
            jnp.where(row_iota == row, one, zero),
            jnp.where(lane_iota == lane, one, zero),
            (((1,), (1,)), ((), ())),
            preferred_element_type=jnp.float32,
        )
    return total


def index_cells(list_ref, mask_ref, base_ref, count_ref, inverse_ref, place_ref, spot_ref):
    mask = draw_mask(list_ref)
    mask_ref[...] = mask
    small = mask.astype(jnp.bfloat16)
    before = lax.broadcasted_iota(jnp.int32, (LANES, LANES), 0) < lax.broadcasted_iota(jnp.int32, (LANES, LANES), 1)
    before = before.astype(jnp.float32).astype(jnp.bfloat16)
    prefix = jnp.dot(small, before, preferred_element_type=jnp.float32).astype(jnp.int32)
    count = jnp.dot(small, jnp.ones((LANES, LANES), jnp.bfloat16), preferred_element_type=jnp.float32).astype(jnp.int32)
    count_ref[...] = count
    most = jnp.zeros((8, LANES), jnp.int32)
    running = most
    for t in range(TILES):
        if t % TEAM == 0:
            running = jnp.zeros((8, LANES), jnp.int32)
        base_ref[8 * t : 8 * t + 8, :] = running
        running = running + count[8 * t : 8 * t + 8]
        most = jnp.maximum(most, running)
    wide_lane = lax.broadcasted_iota(jnp.int32, (FLAT, LANES), 1)
    moved = jnp.where(mask > 0.5, (wide_lane - prefix) * 256 + wide_lane, 0)
    for bit in range(7):
        probe = 256 << bit
        near = pltpu.roll(moved, LANES - (1 << bit), axis=1)
        moved = jnp.where(
            lax.bitwise_and(near, probe) != 0,
            near,
            jnp.where(lax.bitwise_and(moved, probe) != 0, 0, moved),
        )
    inverse = lax.bitwise_and(moved, LANES - 1)
    inverse_ref[...] = inverse
    base = base_ref[...]
    place_ref[...] = jnp.where(mask > 0.5, prefix + base, -1)
    lane = lax.broadcasted_iota(jnp.int32, (8, LANES), 1)
    for t in range(TILES):
        here = slice(8 * t, 8 * t + 8)
        rank = lane - base_ref[here, :]
        inside = jnp.logical_and(rank >= 0, rank < count[here])
        spot = jnp.take_along_axis(inverse[here], jnp.where(inside, rank, 0), axis=1)
        spot_ref[here, :] = jnp.where(inside, spot, -1)
    return jnp.max(most)


def gather_team(picks, kept_ref, snow_ref, single_ref, gathered_ref):
    planes = [(kept_ref, p) for p in range(KEPT)]
    planes += [(snow_ref, p) for p in range(CATS)] + [(single_ref, 0), (single_ref, 1)]
    for start in range(0, len(planes), BLOCK):
        block = planes[start : start + BLOCK]
        values = [None] * len(block)
        for at, spot in picks:
            inside = spot >= 0
            spot = jnp.maximum(spot, 0)
            for k, (ref, p) in enumerate(block):
                value = jnp.take_along_axis(ref[p, at, :], spot, axis=1)
                values[k] = value if values[k] is None else jnp.where(inside, value, values[k])
        for k, value in enumerate(values):
            gathered_ref[start + k] = value


def solve_team(gathered_ref, result_ref):
    air = gathered_ref[KEPT + CATS]
    heat = gathered_ref[KEPT + CATS + 1]
    for cat in range(CATS):
        temps = [gathered_ref[cat * LAYERS + i] for i in range(LAYERS)]
        thick = gathered_ref[STACKED + cat]
        current, growth = column(temps, thick, gathered_ref[KEPT + cat], air)
        for i in range(LAYERS):
            result_ref[cat * LAYERS + i] = current[i]
        result_ref[STACKED + cat] = thick + (growth - 0.0005 * heat)


def field_of(i, moving, forcing):
    return (moving, i) if i < 5 else (forcing, i - 5)


def spread_team(tiles, level, place_ref, source_ref, result_ref, fresh_ref, planes, skip=0):
    for at in tiles:
        place = place_ref[at, :] - level * LANES
        inside = jnp.logical_and(place >= 0, place < LANES)
        spot = jnp.where(inside, place, 0)
        for p in planes:
            value = jnp.take_along_axis(result_ref[p], spot, axis=1)
            fresh_ref[p - skip, at, :] = jnp.where(inside, value, source_ref[p, at, :])


def thermo_kernel(
    list_hbm, temps_hbm, thick_hbm, snow_hbm, area_hbm, air_hbm, heat_hbm,
    vel_hbm, stress_hbm, wind_hbm, ocean_hbm, cells_hbm,
    thick_out, forcing_out, result_out, place_out, left_out, right_out,
    list_ref, kept_ref, fresh_ref, snow_ref, area_ref, single_ref, moving_ref, drive_ref, cells_ref, forcing_ref,
    mask_ref, base_ref, count_ref, inverse_ref, place_ref, spot_ref,
    gathered_a, gathered_b, result_ref, edge_ref, turn_ref, in_sem, out_sem, result_sem, edge_sem, extra_sem,
):
    listing = pltpu.make_async_copy(list_hbm, list_ref, extra_sem)
    listing.start()
    band = lax.axis_index("by")
    north = lax.axis_size("by") * ROWS

    def fetch(turn):
        half, inner = turn // (TURNS // 2), turn % (TURNS // 2)
        span = slice(half * LANES, half * LANES + LANES)
        there = slice(inner * HEIGHT, inner * HEIGHT + HEIGHT)
        rows = slice(turn * HEIGHT, turn * HEIGHT + HEIGHT)
        copies = []
        for source, target in (
            (temps_hbm, kept_ref.at[:STACKED]),
            (thick_hbm, kept_ref.at[STACKED:]),
            (snow_hbm, snow_ref),
            (air_hbm, single_ref.at[0]),
            (heat_hbm, single_ref.at[1]),
            (area_hbm, area_ref),
            (wind_hbm, drive_ref.at[0:2]),
            (ocean_hbm, drive_ref.at[2:4]),
            (cells_hbm, cells_ref),
            (vel_hbm, moving_ref.at[0:2]),
            (stress_hbm, moving_ref.at[2:5]),
        ):
            sem = in_sem.at[turn, len(copies)]
            if len(source.shape) == 3:
                copies.append(pltpu.make_async_copy(source.at[:, there, span], target.at[:, rows, :], sem))
            else:
                copies.append(pltpu.make_async_copy(source.at[there, span], target.at[rows, :], sem))
        return copies

    def send(turn):
        half, inner = turn // (TURNS // 2), turn % (TURNS // 2)
        span = slice(half * LANES, half * LANES + LANES)
        there = slice(inner * HEIGHT, inner * HEIGHT + HEIGHT)
        rows = slice(turn * HEIGHT, turn * HEIGHT + HEIGHT)
        return [
            pltpu.make_async_copy(fresh_ref.at[:, rows, :], thick_out.at[:, there, span], out_sem.at[turn, 0]),
            pltpu.make_async_copy(forcing_ref.at[:, rows, :], forcing_out.at[:, there, span], out_sem.at[turn, 1]),
        ]

    fetched = [fetch(turn) for turn in range(TURNS)]
    for copies in fetched:
        for copy in copies:
            copy.start()
    row = lax.broadcasted_iota(jnp.int32, (ROWS, LANES), 0) + band * ROWS
    latitude = row.astype(jnp.float32) + 0.5
    turn_ref[...] = 1.4 * jnp.sin(0.5 * jnp.pi * (2.0 * latitude / north - 1.0))
    listing.wait()
    most = index_cells(list_ref, mask_ref, base_ref, count_ref, inverse_ref, place_ref, spot_ref)
    sent = [pltpu.make_async_copy(place_ref, place_out, result_sem.at[TILES // TEAM])]
    sent[0].start()
    lane = lax.broadcasted_iota(jnp.int32, (8, LANES), 1)
    buffers = (gathered_a, gathered_b)
    thick_planes = range(STACKED, KEPT)

    def tiles_of(team):
        return [pl.ds(pl.multiple_of((team * TEAM + u) * 8, 8), 8) for u in range(TEAM)]

    def force(turn):
        at = slice(turn * HEIGHT, turn * HEIGHT + HEIGHT)
        ice = mask_ref[at, :]
        load = jnp.zeros(ice.shape, jnp.float32)
        area_total = jnp.zeros(ice.shape, jnp.float32)
        for cat in range(CATS):
            area = area_ref[cat, at, :]
            load = load + area * fresh_ref[cat, at, :]
            area_total = area_total + area
        load = ice * load
        mass = 0.9 * load
        inner = (turn % (TURNS // 2)) * HEIGHT
        turning = turn_ref[inner : inner + HEIGHT, :] * mass
        diagonal = mass + 1.0
        scale = cells_ref[at, :].astype(jnp.float32) / (diagonal * diagonal + turning * turning)
        forcing_ref[0, at, :] = drive_ref[0, at, :] + drive_ref[2, at, :]
        forcing_ref[1, at, :] = drive_ref[1, at, :] + drive_ref[3, at, :]
        forcing_ref[2, at, :] = diagonal * scale
        forcing_ref[3, at, :] = load * jnp.exp(-20.0 * (1.0 - area_total))
        forcing_ref[4, at, :] = mass
        forcing_ref[5, at, :] = turning * scale

    def extra(team):
        def one(level, carry):
            tiles = tiles_of(team)
            picks = []
            for at in tiles:
                rank = lane + level * LANES - base_ref[at, :]
                inside = jnp.logical_and(rank >= 0, rank < count_ref[at, :])
                spot = jnp.take_along_axis(inverse_ref[at, :], jnp.where(inside, rank, 0), axis=1)
                picks.append((at, jnp.where(inside, spot, -1)))
            gather_team(picks, kept_ref, snow_ref, single_ref, gathered_a)
            solve_team(gathered_a, result_ref.at[TILES // TEAM])
            for at in tiles:
                place = place_ref[at, :] - level * LANES
                inside = jnp.logical_and(place >= 0, place < LANES)
                spot = jnp.where(inside, place, 0)
                for p in thick_planes:
                    value = jnp.take_along_axis(result_ref[TILES // TEAM, p], spot, axis=1)
                    fresh_ref[p - STACKED, at, :] = jnp.where(inside, value, fresh_ref[p - STACKED, at, :])
            copy = pltpu.make_async_copy(result_ref.at[TILES // TEAM, :STACKED], result_out.at[level, team], extra_sem)
            copy.start()
            copy.wait()
            return carry

        return one

    for turn in range(TURNS):
        for copy in fetched[turn]:
            copy.wait()
        teams = [turn * PAIR + k for k in range(PAIR)]
        for k, team in enumerate(teams):
            gather_team([(at, spot_ref[at, :]) for at in tiles_of(team)], kept_ref, snow_ref, single_ref, buffers[k % 2])
        for k, team in enumerate(teams):
            solve_team(buffers[k % 2], result_ref.at[team])
        for k, team in enumerate(teams):
            spread_team(tiles_of(team), 0, place_ref, kept_ref, result_ref.at[team], fresh_ref, thick_planes, STACKED)
            copy = pltpu.make_async_copy(result_ref.at[team, :STACKED], result_out.at[0, team], result_sem.at[team])
            copy.start()
            sent.append(copy)
        force(turn)
        for copy in send(turn):
            copy.start()
            sent.append(copy)

    @pl.when(most > LANES)
    def _():
        for copy in sent:
            copy.wait()

        def again(team, carry):
            return lax.fori_loop(1, TEAM, extra(team), carry)

        lax.fori_loop(0, TILES // TEAM, again, 0)
        for turn in range(TURNS):
            force(turn)
        for copy in sent:
            copy.start()

    group = lax.shift_right_logical(lane, 3)
    edges = []
    for half, push, target in ((1, 8, right_out), (0, 0, left_out)):
        for tile in range(ROWS // 8):
            at = slice(8 * tile + half * ROWS, 8 * tile + half * ROWS + 8)
            packed = jnp.zeros((8, LANES), jnp.float32)
            for i in range(FIELDS):
                ref, k = field_of(i, moving_ref, forcing_ref)
                x = ref[k, at, :]
                turn = (8 * i + push) % LANES
                if turn:
                    x = pltpu.roll(x, turn, axis=1)
                packed = jnp.where(group == i, x, packed)
            edge_ref[half, 8 * tile : 8 * tile + 8, :] = packed
        copy = pltpu.make_async_copy(edge_ref.at[half], target, edge_sem.at[half])
        copy.start()
        edges.append(copy)
    for copy in sent + edges:
        copy.wait()


def temps_kernel(half, temps_hbm, result_hbm, place_hbm, *rest):
    temps_out, kept_ref, fresh_ref, place_ref, result_ref, in_sem, out_sem, extra_sem = rest[-8:]
    teams = TILES // TEAM // 2
    height = TEAM * 8
    span = slice(half * LANES, half * LANES + LANES)
    rows = slice(half * ROWS, half * ROWS + ROWS)
    whole = pltpu.make_async_copy(place_hbm.at[rows, :], place_ref, extra_sem)
    whole.start()
    fetched = []
    for k in range(teams):
        here = slice(k * height, k * height + height)
        fetched.append([
            pltpu.make_async_copy(temps_hbm.at[:, here, span], kept_ref.at[:, here, :], in_sem.at[k, 0]),
            pltpu.make_async_copy(result_hbm.at[0, half * teams + k], result_ref.at[k], in_sem.at[k, 1]),
        ])
    for copies in fetched:
        for copy in copies:
            copy.start()
    whole.wait()
    sent = []
    for k in range(teams):
        for copy in fetched[k]:
            copy.wait()
        here = slice(k * height, k * height + height)
        tiles = [slice(k * height + 8 * u, k * height + 8 * u + 8) for u in range(TEAM)]
        spread_team(tiles, 0, place_ref, kept_ref, result_ref.at[k], fresh_ref, range(STACKED))
        copy = pltpu.make_async_copy(fresh_ref.at[:, here, :], temps_out.at[:, here, span], out_sem.at[k])
        copy.start()
        sent.append(copy)

    @pl.when(jnp.max(place_ref[...]) >= LANES)
    def _():
        for copy in sent:
            copy.wait()

        def again(step, carry):
            team = lax.div(step, TEAM - 1)
            level = lax.rem(step, TEAM - 1) + 1
            copy = pltpu.make_async_copy(result_hbm.at[level, half * teams + team], result_ref.at[0], extra_sem)
            copy.start()
            copy.wait()
            for u in range(TEAM):
                at = pl.ds(pl.multiple_of(team * height + 8 * u, 8), 8)
                place = place_ref[at, :] - level * LANES
                inside = jnp.logical_and(place >= 0, place < LANES)
                spot = jnp.where(inside, place, 0)
                for p in range(STACKED):
                    value = jnp.take_along_axis(result_ref[0, p], spot, axis=1)
                    fresh_ref[p, at, :] = jnp.where(inside, value, fresh_ref[p, at, :])
            return carry

        lax.fori_loop(0, teams * (TEAM - 1), again, 0)
        for copy in sent:
            copy.start()

    for copy in sent:
        copy.wait()


def halo_tile(west, east, field, rows):
    lane = lax.broadcasted_iota(jnp.int32, (rows, LANES), 1)
    east_side = pltpu.roll(east, (LANES - 8 * field) % LANES, axis=1) if field else east
    west_side = pltpu.roll(west, (120 - 8 * field) % LANES, axis=1)
    zero = jnp.zeros((rows, LANES), jnp.float32)
    return jnp.where(lane < DEEP, east_side, jnp.where(lane >= LANES - DEEP, west_side, zero))


def rows_kernel(
    vel_low, stress_low, forcing_low, west_low, east_low,
    vel_high, stress_high, forcing_high, west_high, east_high, even_out, odd_out,
):
    even = lax.rem(lax.axis_index("by"), 2) == 0

    def fill(to_low, to_high):
        for out, vel_ref, stress_ref, forcing_ref, west_ref, east_ref in (
            (to_low, vel_low, stress_low, forcing_low, west_low, east_low),
            (to_high, vel_high, stress_high, forcing_high, west_high, east_high),
        ):
            for i in range(FIELDS):
                ref, at = (vel_ref, i) if i < 2 else (stress_ref, i - 2) if i < 5 else (forcing_ref, i - 5)
                out[i, 0] = ref[at, :, :LANES]
                out[i, 1] = ref[at, :, LANES:]
                out[i, 2] = halo_tile(west_ref[...], east_ref[...], i, DEEP)

    @pl.when(even)
    def _():
        fill(odd_out, even_out)

    @pl.when(jnp.logical_not(even))
    def _():
        fill(even_out, odd_out)


def flip(x):
    lane = (LANES - 1) - lax.broadcasted_iota(jnp.int32, (DEEP, LANES), 1)
    turned = jnp.take_along_axis(x, lane, axis=1)
    return jnp.concatenate([turned[i : i + 1] for i in range(DEEP - 1, -1, -1)], axis=0)


def motion_kernel(
    vel_hbm, stress_hbm, forcing_hbm, west_hbm, east_hbm, even_hbm, odd_hbm,
    vel_out, stress_out, state_ref, west_ref, east_ref, even_ref, odd_ref, in_sem, halo_sem, out_sem,
):
    spot = lax.axis_index("by")
    even = lax.rem(spot, 2) == 0
    top = spot == lax.axis_size("by") - 1
    halos = []
    for source, target in ((west_hbm, west_ref), (east_hbm, east_ref), (even_hbm, even_ref), (odd_hbm, odd_ref)):
        copy = pltpu.make_async_copy(source, target, halo_sem.at[len(halos)])
        copy.start()
        halos.append(copy)
    low = slice(DEEP, 2 * DEEP)
    mid = slice(2 * DEEP, 2 * DEEP + ROWS)
    high = slice(2 * DEEP + ROWS, 3 * DEEP + ROWS)
    copies = []
    for tile in range(2):
        span = slice(tile * LANES, tile * LANES + LANES)
        for number, (source, target) in enumerate((
            (vel_hbm, state_ref.at[0:2, tile, mid, :]),
            (stress_hbm, state_ref.at[2:5, tile, mid, :]),
            (forcing_hbm, state_ref.at[5:11, tile, mid, :]),
        )):
            copy = pltpu.make_async_copy(source.at[:, :, span], target, in_sem.at[tile, number])
            copy.start()
            copies.append(copy)
    for copy in halos:
        copy.wait()
    blank = jnp.zeros((DEEP, LANES), jnp.float32)
    for i in range(FIELDS):
        for tile in range(3):
            state_ref[i, tile, :DEEP, :] = blank
            state_ref[i, tile, TALL - DEEP :, :] = blank
        state_ref[i, 2, mid, :] = halo_tile(west_ref[...], east_ref[...], i, ROWS)

    @pl.when(even)
    def _():
        for i in range(FIELDS):
            for tile in range(3):
                state_ref[i, tile, high, :] = even_ref[i, tile]
                state_ref[i, tile, low, :] = odd_ref[i, tile]

    @pl.when(jnp.logical_not(even))
    def _():
        for i in range(FIELDS):
            for tile in range(3):
                state_ref[i, tile, low, :] = even_ref[i, tile]
                state_ref[i, tile, high, :] = odd_ref[i, tile]

    @pl.when(top)
    def _():
        for i in range(FIELDS):
            for tile, source in ((0, 1), (1, 0), (2, 2)):
                turned = flip(odd_ref[i, source])
                state_ref[i, tile, high, :] = -turned if i in (0, 1, 5, 6) else turned

    for copy in copies:
        copy.wait()
    bands = (TALL - 2 * DEEP) // BAND
    lane = lax.broadcasted_iota(jnp.int32, (BAND, LANES), 1)
    is_first = lane == 0
    is_final = lane == LANES - 1

    def shift_x(parts):
        ahead = [pltpu.roll(x, LANES - 1, axis=1) for x in parts]
        behind = [pltpu.roll(x, 1, axis=1) for x in parts]
        return [
            jnp.where(is_final, ahead[(k + 1) % 3], ahead[k]) - jnp.where(is_first, behind[(k + 2) % 3], behind[k])
            for k in range(3)
        ]

    def shift_y(field, tile, start):
        return state_ref[field, tile, pl.ds(start + 1, BAND), :] - state_ref[field, tile, pl.ds(start - 1, BAND), :]

    def stresses(band, carry):
        start = pl.multiple_of(DEEP + band * BAND, 8)
        at = pl.ds(start, BAND)
        east_dx = shift_x([state_ref[0, k, at, :] for k in range(3)])
        north_dx = shift_x([state_ref[1, k, at, :] for k in range(3)])
        for k in range(3):
            north_dy = shift_y(1, k, start)
            diverge = 0.5 * (east_dx[k] + north_dy)
            tension = 0.5 * (east_dx[k] - north_dy)
            shearing = 0.5 * (shift_y(0, k, start) + north_dx[k])
            deform = diverge * diverge + 0.25 * (tension * tension + shearing * shearing) + 1.0
            strength = state_ref[8, k, at, :] * (1.0 / 3.0)
            bulk = strength * lax.rsqrt(deform)
            viscous = bulk * 0.25
            state_ref[2, k, at, :] = state_ref[2, k, at, :] * (2.0 / 3.0) + (bulk * diverge - strength)
            state_ref[3, k, at, :] = state_ref[3, k, at, :] * (2.0 / 3.0) + viscous * tension
            state_ref[4, k, at, :] = state_ref[4, k, at, :] * (2.0 / 3.0) + viscous * (0.5 * shearing)
        return carry

    def momentum(band, carry):
        start = pl.multiple_of(DEEP + band * BAND, 8)
        at = pl.ds(start, BAND)
        up = pl.ds(start + 1, BAND)
        down = pl.ds(start - 1, BAND)
        normal_dx = shift_x([state_ref[2, k, at, :] + state_ref[3, k, at, :] for k in range(3)])
        shear_dx = shift_x([state_ref[4, k, at, :] for k in range(3)])
        for k in range(3):
            shear_dy = shift_y(4, k, start)
            normal_dy = (state_ref[2, k, up, :] - state_ref[3, k, up, :]) - (
                state_ref[2, k, down, :] - state_ref[3, k, down, :]
            )
            mass = state_ref[9, k, at, :]
            right_east = mass * state_ref[0, k, at, :] + (0.25 * normal_dx[k] + 0.5 * shear_dy) + state_ref[5, k, at, :]
            right_north = mass * state_ref[1, k, at, :] + (0.5 * shear_dx[k] + 0.25 * normal_dy) + state_ref[6, k, at, :]
            straight = state_ref[7, k, at, :]
            turned = state_ref[10, k, at, :]
            state_ref[0, k, at, :] = straight * right_east + turned * right_north
            state_ref[1, k, at, :] = straight * right_north - turned * right_east
        return carry

    def subcycle(turn, carry):
        lax.fori_loop(0, bands, stresses, 0)
        lax.fori_loop(0, bands, momentum, 0)
        return carry

    lax.fori_loop(0, SUB - 1, subcycle, 0)
    lax.fori_loop(0, bands, stresses, 0)
    sent = []

    def send(number, fields, target):
        for tile in range(2):
            span = slice(tile * LANES, tile * LANES + LANES)
            copy = pltpu.make_async_copy(
                state_ref.at[fields, tile, mid, :], target.at[:, :, span], out_sem.at[tile, number]
            )
            copy.start()
            sent.append(copy)

    send(0, slice(2, 5), stress_out)
    lax.fori_loop(0, bands, momentum, 0)
    send(1, slice(0, 2), vel_out)
    for copy in sent:
        copy.wait()


def per_device(
    layer_temps, ice_thick, snow_thick, ice_area, air_temp, ocean_heat,
    velocity, stress, wind_stress, ocean_current, ocean_mask, ice_cols,
):
    f32 = jnp.float32
    i32 = jnp.int32
    here = pl.BlockSpec(memory_space=pl.ANY)
    listed = ice_cols.reshape(1, -1)

    def flat(n, kind=f32):
        return pltpu.VMEM((n, FLAT, LANES), kind)

    one = pltpu.VMEM((FLAT, LANES), i32)
    teams = TILES // TEAM
    thick_new, forcing, result, place, left, right = pl.pallas_call(
        thermo_kernel,
        name="thermo",
        in_specs=[here] * 12,
        out_specs=[here] * 6,
        out_shape=[
            jax.ShapeDtypeStruct((CATS, ROWS, COLS), f32),
            jax.ShapeDtypeStruct((6, ROWS, COLS), f32),
            jax.ShapeDtypeStruct((TEAM, teams, STACKED, 8, LANES), f32),
            jax.ShapeDtypeStruct((FLAT, LANES), i32),
            jax.ShapeDtypeStruct((ROWS, LANES), f32),
            jax.ShapeDtypeStruct((ROWS, LANES), f32),
        ],
        scratch_shapes=[
            pltpu.VMEM(listed.shape, i32),
            flat(KEPT), flat(CATS), flat(CATS), flat(CATS), flat(2), flat(5), flat(4), one, flat(6),
            pltpu.VMEM((FLAT, LANES), f32), one, one, one, one, one,
            pltpu.VMEM((KEPT + CATS + 2, 8, LANES), f32),
            pltpu.VMEM((KEPT + CATS + 2, 8, LANES), f32),
            pltpu.VMEM((teams + 1, KEPT, 8, LANES), f32),
            pltpu.VMEM((2, ROWS, LANES), f32),
            pltpu.VMEM((ROWS, LANES), f32),
            pltpu.SemaphoreType.DMA((TURNS, 11)),
            pltpu.SemaphoreType.DMA((TURNS, 2)),
            pltpu.SemaphoreType.DMA((teams + 1,)),
            pltpu.SemaphoreType.DMA((2,)),
            pltpu.SemaphoreType.DMA,
        ],
    )(
        listed, layer_temps, ice_thick, snow_thick, ice_area, air_temp, ocean_heat,
        velocity, stress, wind_stress, ocean_current, ocean_mask,
    )

    def renew(half, *before):
        return pl.pallas_call(
            functools.partial(temps_kernel, half),
            name="temps_west" if half == 0 else "temps_east",
            in_specs=[here] * (3 + len(before)),
            out_specs=here,
            out_shape=jax.ShapeDtypeStruct((STACKED, ROWS, COLS), f32),
            input_output_aliases={3: 0} if before else {},
            cost_estimate=pl.CostEstimate(flops=20_000_000, transcendentals=0, bytes_accessed=6_000_000),
            scratch_shapes=[
                pltpu.VMEM((STACKED, ROWS, LANES), f32),
                pltpu.VMEM((STACKED, ROWS, LANES), f32),
                pltpu.VMEM((ROWS, LANES), i32),
                pltpu.VMEM((teams // 2, STACKED, 8, LANES), f32),
                pltpu.SemaphoreType.DMA((teams // 2, 2)),
                pltpu.SemaphoreType.DMA((teams // 2,)),
                pltpu.SemaphoreType.DMA,
            ],
        )(layer_temps, result, place, *before)

    n_bx = lax.axis_size("bx")
    n_by = lax.axis_size("by")
    west = lax.ppermute(right, "bx", [(q, (q + 1) % n_bx) for q in range(n_bx)])
    east = lax.ppermute(left, "bx", [((q + 1) % n_bx, q) for q in range(n_bx)])
    temps_part = renew(0)
    band = jax.ShapeDtypeStruct((FIELDS, 3, DEEP, LANES), f32)

    def slab(n, block):
        return pl.BlockSpec((n, DEEP, COLS), lambda i: (0, block, 0))

    def edge(block):
        return pl.BlockSpec((DEEP, LANES), lambda i: (block, 0))

    final = ROWS // DEEP - 1
    halo = pl.BlockSpec((FIELDS, 3, DEEP, LANES), lambda i: (0, 0, 0, 0))
    even_rows, odd_rows = pl.pallas_call(
        rows_kernel,
        name="edge_rows",
        grid=(1,),
        in_specs=[slab(2, 0), slab(3, 0), slab(6, 0), edge(0), edge(0)]
        + [slab(2, final), slab(3, final), slab(6, final), edge(final), edge(final)],
        out_specs=[halo, halo],
        out_shape=[band, band],
    )(velocity, stress, forcing, west, east, velocity, stress, forcing, west, east)

    def at(p, q):
        return q * n_by + p

    even_pairs, odd_pairs = [], []
    for q in range(n_bx):
        for p in range(0, n_by, 2):
            even_pairs += [(at(p, q), at(p + 1, q)), (at(p + 1, q), at(p, q))]
        for p in range(1, n_by - 1, 2):
            odd_pairs += [(at(p, q), at(p + 1, q)), (at(p + 1, q), at(p, q))]
        odd_pairs.append((at(n_by - 1, q), at(n_by - 1, n_bx - 1 - q)))
    even_rows, odd_rows, temps_part = lax.optimization_barrier((even_rows, odd_rows, temps_part))
    odd_halo = lax.ppermute(odd_rows, ("bx", "by"), odd_pairs)
    even_halo = lax.ppermute(even_rows, ("bx", "by"), even_pairs)
    temps_new = renew(1, temps_part)
    edge_shape = pltpu.VMEM((ROWS, LANES), f32)
    band_shape = pltpu.VMEM((FIELDS, 3, DEEP, LANES), f32)
    velocity_new, stress_new = pl.pallas_call(
        motion_kernel,
        name="motion",
        in_specs=[here] * 7,
        out_specs=[here, here],
        out_shape=[
            jax.ShapeDtypeStruct((2, ROWS, COLS), f32),
            jax.ShapeDtypeStruct((3, ROWS, COLS), f32),
        ],
        scratch_shapes=[
            pltpu.VMEM((FIELDS, 3, TALL, LANES), f32),
            edge_shape, edge_shape, band_shape, band_shape,
            pltpu.SemaphoreType.DMA((2, 3)),
            pltpu.SemaphoreType.DMA((4,)),
            pltpu.SemaphoreType.DMA((2, 2)),
        ],
    )(velocity, stress, forcing, west, east, even_halo, odd_halo)
    return temps_new, thick_new, velocity_new, stress_new


def solution(mesh):
    grid3 = P(None, "by", "bx")
    grid2 = P("by", "bx")
    in_specs = (
        grid3, grid3, grid3, grid3, grid2, grid2, grid3, grid3, grid3, grid3, grid2,
        P("by", "bx", None),
    )
    return jax.shard_map(
        per_device, mesh=mesh, in_specs=in_specs, out_specs=(grid3,) * 4, check_vma=False
    )
```
